256 devices in a mesh: parts: 2 (over y), seq: 16 (over z), head: 4 (over x), rep: 2 (over core).
Axes of the slice: x: 4, y: 2, z: 16, core: 2. Of those that a mesh axis runs over, the one named last changes fastest.
The devices are a block of a 4x16x16 slice.
Arguments:
- queries: bfloat16 [4, 4096, 2048], P(('parts', 'rep'), 'seq', 'head'), parts along dimension 0, may hold values from -6 to 6
- reflect_keys: bfloat16 [4, 4096, 2, 2048], P(('parts', 'rep'), 'seq', None, 'head'), parts along dimension 0, may hold values from -6 to 6
- reflect_values: bfloat16 [4, 4096, 2, 2048], P(('parts', 'rep'), 'seq', None, 'head'), parts along dimension 0, may hold values from -6 to 6
- reflect_beta: float32 [4, 4096, 2, 16], P(('parts', 'rep'), 'seq', None, 'head'), parts along dimension 0, may hold values from 0.2 to 2
- log_decay: float32 [4, 4096, 16], P(('parts', 'rep'), 'seq', 'head'), parts along dimension 0, may hold values from -2.5 to 0
- prompt_lengths: int32 [4, 6], P(('parts', 'rep')), parts along dimension 0, may hold values from 1 to 2048, 4096 in all within a row
- norm_gain: float32 [128], replicated, may hold values from 0.1 to 1.9
- out_weight: bfloat16 [2048, 2048], P('head'), may hold values from -0.125 to 0.125
Outputs:
- layer_out: bfloat16 [4, 4096, 2048], P(('parts', 'rep'), ('seq', 'head')), parts along dimension 0
The draws below stay inside these ranges and needn't reach their ends.
There are 2 independent parts, one for each index of `parts`. The reference program is written for one: setup_inputs(seed, part) draws one part's arguments, and reference() takes and returns one part's arrays. A program takes and returns all parts, laid end to end along the dimension named above; an argument that names none is the same for every part. Nothing has to cross between parts.
Inputs may be any that keep to these rules, and one draw needn't show every extreme that they name: `prompt_lengths`: the 6 prompts of a pack lie end to end from its first token and cover all 4096 tokens; the longest has exactly 2048.
All inputs are finite; a program needn't handle non-finite values.
Results may differ from the reference program's by a relative error of at most 0.0095.
Values may be sent and summed in bfloat16 or wider, within the bound.
No kernel may reach another device: no remote copies, remote signals or barrier semaphores. Data moves between devices by JAX's collectives and lax.ppermute only.
A program may use at most 64 MiB of HBM per device.

```python
import math
import jax
import jax.numpy as jnp
import numpy as np
from jax import lax

D = 2048
HEADS = 16
DK = 128
REFL = 2
BLOCK = 64
DOCS = 6
TOK_DEV = 256
BUNDLE_COUNT = 2
BUNDLE_SPAN = 4096
MOST_LEN = 2048
N_HEAD = 4


def slow_heads(key):
    chances = jax.random.uniform(jax.random.fold_in(key, 11), (HEADS,))
    return chances < 0.5


def draw_log_decay(key, part):
    slow_mask = slow_heads(key)
    slow_rate = jnp.exp(jax.random.uniform(jax.random.fold_in(key, 21), (HEADS,), minval=jnp.log(0.1 / MOST_LEN), maxval=jnp.log(1.0 / MOST_LEN)))
    fast_rate = jnp.exp(jax.random.uniform(jax.random.fold_in(key, 22), (HEADS,), minval=jnp.log(1.0 / 50.0), maxval=jnp.log(1.0 / 20.0)))
    channel_speed = jnp.where(slow_mask, slow_rate, fast_rate)
    uneven_quantity = jax.random.uniform(jax.random.fold_in(key, 23), (BUNDLE_COUNT, BUNDLE_SPAN, HEADS), minval=0.4, maxval=1.6)
    symbol_span = jnp.exp(jax.random.uniform(jax.random.fold_in(key, 24), (BUNDLE_COUNT, BUNDLE_SPAN // TOK_DEV, HEADS), minval=jnp.log(0.5), maxval=jnp.log(2.0)))
    symbol_span = jnp.repeat(symbol_span, TOK_DEV, axis=1)
    spike_position = jax.random.randint(jax.random.fold_in(key, 25), (BUNDLE_COUNT, 3), 0, BUNDLE_SPAN)
    spike_kept = jax.random.uniform(jax.random.fold_in(key, 26), (BUNDLE_COUNT, 3), minval=0.5, maxval=0.8)
    spike_hits = jnp.arange(BUNDLE_SPAN)[None, None, :] == spike_position[:, :, None]
    spike_log_scale = jnp.sum(jnp.where(spike_hits, jnp.log(spike_kept)[:, :, None], 0.0), axis=1)
    return (spike_log_scale[:, :, None] - channel_speed * uneven_quantity * symbol_span).astype(jnp.float32)


def draw_reflect_beta(key, part):
    slow_mask = slow_heads(key)
    margin = jnp.exp(jax.random.uniform(jax.random.fold_in(key, 31), (BUNDLE_COUNT, BUNDLE_SPAN, REFL, HEADS), minval=jnp.log(0.0001), maxval=jnp.log(0.02)))
    spread = jax.random.uniform(jax.random.fold_in(key, 32), (BUNDLE_COUNT, BUNDLE_SPAN, REFL, HEADS), minval=0.2, maxval=1.9)
    return jnp.where(slow_mask, 2.0 - margin, spread).astype(jnp.float32)


def shard_levels(rng, shape, pieces, least, top_value):
    gain, own = 1.0, jax.random.fold_in(rng, 6)
    for position, blocks in pieces:
        draws = jnp.exp(jax.random.uniform(jax.random.fold_in(own, position), (blocks,), jnp.float32, least / len(pieces), top_value / len(pieces)))
        gain = gain * jnp.repeat(draws, shape[position] // blocks).reshape([-1 if axis == position else 1 for axis in range(len(shape))])
    return gain


def profile(amount, total, reach, skew):
    loads = [(1 << 20) // math.isqrt(standing ** skew) + 1 for standing in range(2, amount + 1)]
    rest, holding = total - reach - (amount - 1), [1] * (amount - 1)
    while rest > 0:
        candidates = [i for i in range(amount - 1) if holding[i] < reach]
        pool, budget = sum([loads[i] for i in candidates]), rest
        for i in candidates:
            extra = min(reach - holding[i], max(1, budget * loads[i] // pool), rest)
            holding[i] = holding[i] + extra
            rest = rest - extra
    return np.array([reach] + holding)


def ragged(rng, count, total, limit, lean):
    if count == 2:
        one = jax.random.randint(rng, (), max(1, total - limit), min(limit, total - 1) + 1)
        return jnp.stack([one, total - one])
    tallies = jnp.asarray(profile(count, total, limit, lean), jnp.int32)
    twos = (count - 1) // 2
    donor, taker = tallies[1:1 + 2 * twos:2], tallies[2:2 + 2 * twos:2]
    room = jnp.minimum(donor - 1, limit - taker)
    moved = jax.random.randint(jax.random.fold_in(rng, 1), (twos,), 0, 1 << 20) % (room + 1)
    tallies = tallies.at[1:1 + 2 * twos:2].set(donor - moved).at[2:2 + 2 * twos:2].set(taker + moved)
    return tallies[jax.random.permutation(jax.random.fold_in(rng, 2), count)]


def scatter_about(key, extent, width, most, cuts=(), held_as=jnp.bfloat16):
    factor_of = shard_levels(key, extent, cuts, -0.22, 0.18) if cuts else 1.0
    entries = jax.random.normal(key, extent, jnp.float32) * width * factor_of
    return jnp.minimum(jnp.maximum(entries, -most), most).astype(held_as)


def setup_inputs(seed: int = 0, part: int = 0) -> dict:
    streams_of = jax.random.split(jax.random.key(seed), 9)
    own_keys = jax.random.split(jax.random.fold_in(streams_of[8], part), 9)
    queries = scatter_about(own_keys[0], (BUNDLE_COUNT, BUNDLE_SPAN, HEADS * DK), 1.0, 6.0, ((0, 2), (1, 16), (2, 4)))
    reflect_keys = scatter_about(own_keys[1], (BUNDLE_COUNT, BUNDLE_SPAN, REFL, HEADS * DK), 1.0, 6.0, ((0, 2), (1, 16), (3, 4)))
    reflect_values = scatter_about(own_keys[2], (BUNDLE_COUNT, BUNDLE_SPAN, REFL, HEADS * DK), 1.0, 6.0, ((0, 2), (1, 16), (3, 4)))
    reflect_beta = draw_reflect_beta(jax.random.fold_in(jax.random.fold_in(streams_of[8], part), 71), part)
    log_decay = draw_log_decay(jax.random.fold_in(jax.random.fold_in(streams_of[8], part), 71), part)
    prompt_lengths = jax.vmap(lambda own: ragged(own, DOCS, BUNDLE_SPAN, MOST_LEN, 2))(jax.random.split(own_keys[5], BUNDLE_COUNT)).reshape((BUNDLE_COUNT, DOCS)).astype(jnp.int32)
    norm_gain = jnp.clip(1.0 + 0.18 * jax.random.normal(streams_of[6], (DK,), jnp.float32), 0.1, 1.9)
    out_weight = scatter_about(streams_of[7], (HEADS * DK, D), (HEADS * DK) ** -0.5, 0.125, ((0, 4),))
    return dict(queries=queries, reflect_keys=reflect_keys, reflect_values=reflect_values, reflect_beta=reflect_beta, log_decay=log_decay, prompt_lengths=prompt_lengths, norm_gain=norm_gain, out_weight=out_weight)


highest = lax.Precision.HIGHEST
epsilon = 1e-06

def unit_rows(vectors):
    return vectors * lax.rsqrt(lax.optimization_barrier(jnp.sum(vectors * vectors, axis=-1, keepdims=True)) + epsilon)

def block_parts(key_rows, value_rows, beta_rows, decay_rows, seg_rows, seg_before):
    steps_here = key_rows.shape[-2]
    cum_decay = jnp.cumsum(decay_rows, axis=-1)
    ordinal = jnp.arange(steps_here)
    incl_mask = ordinal[:, None] >= ordinal[None, :]
    strict_mask = ordinal[:, None] > ordinal[None, :]
    same_doc = seg_rows[:, None, :, None] == seg_rows[:, None, None, :]
    decay_gap = cum_decay[..., :, None] - cum_decay[..., None, :]
    decay_ratio = jnp.where(incl_mask & same_doc, jnp.exp(jnp.minimum(decay_gap, 0.0)), 0.0)
    carry_in = jnp.where(seg_rows[:, None, :] == seg_before[:, None, None], jnp.exp(cum_decay), 0.0)
    key_inner = jnp.einsum('bhik,bhjk->bhij', key_rows, key_rows, precision=highest)
    system = jnp.eye(steps_here, dtype=key_rows.dtype) + jnp.where(strict_mask, beta_rows[..., :, None] * decay_ratio * key_inner, 0.0)
    right_side = jnp.concatenate([beta_rows[..., None] * value_rows, (beta_rows * carry_in)[..., None] * key_rows], axis=-1)
    solved = lax.linalg.triangular_solve(system, right_side, left_side=True, lower=True, unit_diagonal=True)
    val_width = value_rows.shape[-1]
    return (decay_ratio, carry_in, solved[..., :val_width], solved[..., val_width:])

def reference(queries, reflect_keys, reflect_values, reflect_beta, log_decay, prompt_lengths, norm_gain, out_weight):
    pack_count = queries.shape[0]
    length = queries.shape[1]
    blocks = length // BLOCK
    sub_steps = REFL * BLOCK
    doc_ends = jnp.cumsum(prompt_lengths, axis=-1).astype(jnp.int32)
    positions = jnp.arange(length, dtype=jnp.int32)
    segment = lax.optimization_barrier(jnp.sum((positions[None, :, None] >= doc_ends[:, None, :]).astype(jnp.int32), axis=-1)).astype(jnp.int32)
    query_rows = unit_rows(queries.astype(jnp.float32).reshape(pack_count, blocks, BLOCK, HEADS, DK)) * DK ** (-0.5)
    query_rows = query_rows.transpose(1, 0, 3, 2, 4)
    key_rows = unit_rows(reflect_keys.astype(jnp.float32).reshape(pack_count, blocks, BLOCK, REFL, HEADS, DK))
    key_rows = key_rows.transpose(1, 0, 4, 2, 3, 5).reshape(blocks, pack_count, HEADS, sub_steps, DK)
    value_rows = reflect_values.astype(jnp.float32).reshape(pack_count, blocks, BLOCK, REFL, HEADS, DK)
    value_rows = value_rows.transpose(1, 0, 4, 2, 3, 5).reshape(blocks, pack_count, HEADS, sub_steps, DK)
    beta_rows = reflect_beta.reshape(pack_count, blocks, BLOCK, REFL, HEADS).transpose(1, 0, 4, 2, 3).reshape(blocks, pack_count, HEADS, sub_steps)
    gate_rows = log_decay.reshape(pack_count, blocks, BLOCK, HEADS).transpose(1, 0, 3, 2)
    decay_rows = jnp.concatenate([gate_rows[..., None], jnp.zeros(gate_rows.shape + (REFL - 1,), jnp.float32)], axis=-1).reshape(blocks, pack_count, HEADS, sub_steps)
    seg_rows = jnp.repeat(segment.reshape(pack_count, blocks, BLOCK), REFL, axis=-1).transpose(1, 0, 2).astype(jnp.int32)
    last_row = REFL - 1

    def one_block(carried, inputs):
        state, seg_before = carried
        query_block, key_block, value_block, beta_block, decay_block, seg_block = inputs
        decay_ratio, carry_in, write_vals, write_keys = block_parts(key_block, value_block, beta_block, decay_block, seg_block, seg_before)
        updates = write_vals - jnp.einsum('bhck,bhkv->bhcv', write_keys, state, precision=highest)
        read_weights = decay_ratio[..., last_row::REFL, :] * jnp.einsum('bhik,bhjk->bhij', query_block, key_block, precision=highest)
        carry_read = carry_in[..., last_row::REFL]
        head_out = carry_read[..., None] * jnp.einsum('bhik,bhkv->bhiv', query_block, state, precision=highest) + jnp.einsum('bhij,bhjv->bhiv', read_weights, updates, precision=highest)
        end_keys = decay_ratio[..., -1, :, None] * key_block
        new_state = carry_in[..., -1, None, None] * state + jnp.einsum('bhjk,bhjl->bhkl', end_keys, updates, precision=highest)
        return ((new_state, seg_block[:, -1].astype(jnp.int32)), head_out)
    initial = (jnp.zeros((pack_count, HEADS, DK, DK), jnp.float32), jnp.full((pack_count,), -1, jnp.int32))
    finished, outputs = lax.scan(one_block, initial, (query_rows, key_rows, value_rows, beta_rows, decay_rows, seg_rows))
    outputs = outputs.transpose(1, 0, 3, 2, 4)
    normed = (outputs * lax.rsqrt(lax.optimization_barrier(jnp.mean(outputs * outputs, axis=-1, keepdims=True)) + epsilon) * norm_gain).astype(jnp.bfloat16)
    flat_rows = normed.reshape(pack_count, length, HEADS * DK)
    group_width = HEADS * DK // N_HEAD
    total_sum = jnp.zeros((pack_count, length, out_weight.shape[1]), jnp.float32)
    for group_index in range(N_HEAD):
        lower_col = group_index * group_width
        upper_col = lower_col + group_width
        partial_sum = jnp.dot(flat_rows[..., lower_col:upper_col].astype(jnp.float32), out_weight[lower_col:upper_col].astype(jnp.float32), preferred_element_type=jnp.float32).astype(jnp.bfloat16)
        partial_sum = lax.optimization_barrier(partial_sum)
        total_sum = total_sum + partial_sum.astype(jnp.float32)
    return total_sum.astype(jnp.bfloat16)
```

```python
import jax
import jax.numpy as jnp
from jax import lax
from jax.experimental import pallas as pl
from jax.experimental.pallas import tpu as pltpu
from jax.sharding import PartitionSpec as P

BLOCK = 64
MOST_LEN = 2048
epsilon = 1e-06
f32 = jnp.float32
bf16 = jnp.bfloat16


def dot_nn(left, right):
    return lax.dot_general(left, right, (((1,), (0,)), ((), ())), preferred_element_type=f32)


def dot_nt(left, right):
    return lax.dot_general(left, right, (((1,), (1,)), ((), ())), preferred_element_type=f32)


def dot_tn(left, right):
    return lax.dot_general(left, right, (((0,), (0,)), ((), ())), preferred_element_type=f32)


def halves(value):
    top = value.astype(bf16)
    return top, (value - top.astype(f32)).astype(bf16)


def square_product(left, right):
    width = right[0].shape[1]
    side = jnp.concatenate([right[0], right[1]], axis=1)
    both = dot_nn(
        jnp.concatenate([left[0], left[1]], axis=1), jnp.concatenate([side, side], axis=0)
    )
    return both[:, :width] + both[:, width:]


def iota(shape, dim):
    return lax.broadcasted_iota(jnp.int32, shape, dim)


def local_kernel(
    lengths, query, keys, values, beta, decay, reads, offsets, maps, adds, whole_map, whole_add
):
    head = pl.program_id(0)
    tokens = query.shape[1]
    width = query.shape[2]
    refl = keys.shape[2]
    steps = BLOCK * refl
    blocks = tokens // BLOCK
    first = lax.axis_index("seq") * tokens
    ends, end = [], jnp.int32(0)
    for doc in range(lengths.shape[1]):
        end = end + lengths[0, doc]
        ends.append(end)

    def start_of(position):
        start = jnp.zeros_like(position)
        for end in ends:
            start = jnp.where(end <= position, end, start)
        return start

    key_all = keys[0].reshape(tokens * refl, width)
    value_all = values[0].reshape(tokens * refl, width)
    row = iota((steps, steps), 0)
    col = iota((steps, steps), 1)
    eye = row == col
    incl = col <= row
    strict = col < row
    unit = jnp.where(eye, 1.0, 0.0).astype(f32)
    step_col = iota((steps, 1), 0)
    token_col = step_col // refl
    refl_col = step_col % refl
    token_lane = iota((steps, BLOCK), 1)
    read_col = iota((BLOCK, 1), 0)
    read_lane = iota((BLOCK, BLOCK), 1)
    read_step = iota((BLOCK, steps), 1)

    def to_row(column):
        return jnp.sum(jnp.where(eye, column, 0.0), axis=0, keepdims=True)

    gate_all = decay[pl.ds(head, 1), :]
    beta_all = [beta[j, pl.ds(head, 1), :] for j in range(refl)]
    chains = []
    for block in range(blocks):
        at = block * BLOCK
        begin = first + at
        key = key_all[at * refl : at * refl + steps]
        gate = gate_all[:, at : at + BLOCK]
        cum = jnp.sum(jnp.where(token_lane <= token_col, gate, 0.0), axis=1, keepdims=True)
        beta_here = beta_all[refl - 1][:, at : at + BLOCK]
        for j in range(refl - 1):
            beta_here = jnp.where(refl_col == j, beta_all[j][:, at : at + BLOCK], beta_here)
        strength = jnp.sum(
            jnp.where(token_lane == token_col, beta_here, 0.0), axis=1, keepdims=True
        )
        start = start_of(begin + token_col)
        gram = dot_nt(key, key)
        diagonal = jnp.where(eye, gram, 0.0)
        scale = lax.rsqrt(jnp.sum(diagonal, axis=1, keepdims=True) + epsilon)
        scale_row = lax.rsqrt(jnp.sum(diagonal, axis=0, keepdims=True) + epsilon)
        carry = jnp.where(start < begin, jnp.exp(cum), 0.0)
        cum_row = to_row(cum)
        ratio = jnp.where(
            strict & (begin + col // refl >= start),
            jnp.exp(jnp.minimum(cum - cum_row, 0.0)),
            0.0,
        )
        system = (strength * scale) * ratio * gram * scale_row
        chains.append(
            dict(
                at=at,
                begin=begin,
                key=key,
                gate=gate,
                cum=cum,
                cum_row=cum_row,
                strength=strength,
                scale=scale,
                scale_row=scale_row,
                carry=carry,
                system=halves(system),
                inverse=unit - jnp.where((row ^ col) == 1, system, 0.0),
            )
        )
    size = 2
    while size < steps:
        mask = ((row // size) ^ (col // size)) == 1
        for c in chains:
            inverse = halves(c["inverse"])
            corner = tuple(
                jnp.where(mask, part, jnp.zeros_like(part)) for part in c["system"]
            )
            moved = square_product(corner, inverse)
            c["inverse"] = c["inverse"] - square_product(inverse, halves(moved))
        size *= 2
    total = None
    for block, c in enumerate(chains):
        at, begin, key, cum = c["at"], c["begin"], c["key"], c["cum"]
        value = value_all[at * refl : at * refl + steps]
        strength_row = to_row(c["strength"])
        carry_row = to_row(c["carry"])
        value_side = jnp.concatenate(halves(c["inverse"] * strength_row), axis=1)
        key_side = jnp.concatenate(
            halves(c["inverse"] * (strength_row * carry_row * c["scale_row"])), axis=1
        )
        writes = jnp.concatenate(
            [
                dot_nn(value_side, jnp.concatenate([value, value], axis=0)),
                dot_nn(key_side, jnp.concatenate([key, key], axis=0)),
            ],
            axis=1,
        )
        last = begin + BLOCK - 1
        last_start = start_of(last)
        fade = c["scale"] * jnp.where(
            begin + token_col >= last_start,
            jnp.exp(jnp.minimum(cum[steps - 1 :, :] - cum, 0.0)),
            0.0,
        )
        faded = jnp.concatenate(halves(fade * writes), axis=0)
        summed = dot_tn(jnp.concatenate([key, key], axis=0), faded)
        block_add = summed[:, :width]
        block_map = c["carry"][steps - 1 :, :] * unit - summed[:, width:]
        query_here = query[0, at : at + BLOCK, :]
        query_f = query_here.astype(f32)
        query_scale = lax.rsqrt(
            jnp.sum(query_f * query_f, axis=1, keepdims=True) + epsilon
        ) * (width ** (-0.5))
        read_cum = jnp.sum(jnp.where(read_lane <= read_col, c["gate"], 0.0), axis=1, keepdims=True)
        read_start = start_of(begin + read_col)
        read_token = read_step // refl
        weights = jnp.where(
            (read_token <= read_col) & (begin + read_token >= read_start),
            jnp.exp(jnp.minimum(read_cum - c["cum_row"], 0.0)),
            0.0,
        )
        weights = weights * dot_nt(query_here, key) * query_scale * c["scale_row"]
        writes_top = writes.astype(bf16)
        seen = dot_nn(
            jnp.concatenate(halves(weights), axis=1),
            jnp.concatenate([writes_top, writes_top], axis=0),
        )
        read_carry = jnp.where(read_start < begin, jnp.exp(read_cum), 0.0)
        offsets[0, at : at + BLOCK, :] = seen[:, :width]
        reads[0, at : at + BLOCK, :] = (
            (read_carry * query_scale) * query_f - seen[:, width:]
        ).astype(bf16)
        maps[0, block] = block_map.astype(bf16)
        adds[0, block] = block_add
        if total is None:
            total = jnp.concatenate([block_map, block_add], axis=1)
        else:
            top, low = halves(block_map)
            tall = jnp.concatenate(
                [
                    jnp.concatenate([top, top], axis=1),
                    jnp.concatenate([low, jnp.zeros_like(low)], axis=1),
                ],
                axis=0,
            )
            joined = dot_nn(tall, jnp.concatenate(halves(total), axis=0))
            joined = joined[:width] + joined[width:]
            total = jnp.concatenate(
                [joined[:, :width], joined[:, width:] + block_add], axis=1
            )
    whole_map[0] = total[:, :width].astype(bf16)
    whole_add[0] = total[:, width:]


def final_kernel(
    lo_state, hi_state, reads, offsets, maps, adds, gain, weight, *rest
):
    outs, normed = rest[:-1], rest[-1]
    heads, tokens, width = reads.shape
    blocks = tokens // BLOCK
    half = lo_state.shape[0]
    for head in range(heads):
        state = lo_state[head] if head < half else hi_state[head - half]
        for block in range(blocks):
            at = block * BLOCK
            out = dot_nn(reads[head, at : at + BLOCK, :], state) + offsets[head, at : at + BLOCK, :]
            out = out * lax.rsqrt(jnp.mean(out * out, axis=1, keepdims=True) + epsilon)
            normed[at : at + BLOCK, head * width : (head + 1) * width] = (
                out * gain[...]
            ).astype(bf16)
            if block + 1 < blocks:
                state = (dot_nn(maps[head, block], state) + adds[head, block]).astype(bf16)
    peers = len(outs)
    rows = tokens // peers
    me = lax.axis_index("head")
    for turn in range(peers):
        chunk = lax.rem(me + turn, peers)
        here = normed[pl.ds(chunk * rows, rows), :]
        outs[turn][...] = dot_nn(here, weight[...]).astype(bf16)


def shifted(value, axis, steps):
    count = lax.axis_size(axis)
    return lax.ppermute(value, axis, [(source, source + steps) for source in range(count - steps)])


def rotated(value, axis, steps):
    count = lax.axis_size(axis)
    return lax.ppermute(value, axis, [(source, (source + steps) % count) for source in range(count)])


def body(
    queries,
    reflect_keys,
    reflect_values,
    reflect_beta,
    log_decay,
    prompt_lengths,
    norm_gain,
    out_weight,
):
    tokens = queries.shape[1]
    refl = reflect_keys.shape[2]
    heads = reflect_beta.shape[3]
    width = queries.shape[2] // heads
    blocks = tokens // BLOCK
    beta = reflect_beta[0].transpose(1, 2, 0)
    decay = log_decay[0].transpose(1, 0)
    rows_spec = pl.BlockSpec((1, tokens, width), lambda h: (h, 0, 0))
    square_spec = pl.BlockSpec((1, blocks, width, width), lambda h: (h, 0, 0, 0))
    whole_spec = pl.BlockSpec((1, width, width), lambda h: (h, 0, 0))
    reads, offsets, maps, adds, whole_map, whole_add = pl.pallas_call(
        local_kernel,
        grid=(heads,),
        in_specs=[
            pl.BlockSpec(memory_space=pltpu.SMEM),
            pl.BlockSpec((1, tokens, width), lambda h: (0, 0, h)),
            pl.BlockSpec((1, tokens, refl, width), lambda h: (0, 0, 0, h)),
            pl.BlockSpec((1, tokens, refl, width), lambda h: (0, 0, 0, h)),
            pl.BlockSpec((refl, heads, tokens), lambda h: (0, 0, 0)),
            pl.BlockSpec((heads, tokens), lambda h: (0, 0)),
        ],
        out_specs=[rows_spec, rows_spec, square_spec, square_spec, whole_spec, whole_spec],
        out_shape=[
            jax.ShapeDtypeStruct((heads, tokens, width), bf16),
            jax.ShapeDtypeStruct((heads, tokens, width), f32),
            jax.ShapeDtypeStruct((heads, blocks, width, width), bf16),
            jax.ShapeDtypeStruct((heads, blocks, width, width), f32),
            jax.ShapeDtypeStruct((heads, width, width), bf16),
            jax.ShapeDtypeStruct((heads, width, width), f32),
        ],
        name="local_blocks",
    )(prompt_lengths, queries, reflect_keys, reflect_values, beta, decay)

    hops = min(lax.axis_size("seq") - 1, -(-(MOST_LEN - 1) // tokens))
    half = heads // 2
    parts = [slice(0, half), slice(half, heads)]
    part_maps = [whole_map[p] for p in parts]
    part_adds = [whole_add[p] for p in parts]
    states = [shifted(add.astype(bf16), "seq", 1) for add in part_adds]
    for hop in range(hops - 1):
        sent = [
            (
                jnp.einsum("hij,hjk->hik", m, s, preferred_element_type=f32) + a
            ).astype(bf16)
            for m, s, a in zip(part_maps, states, part_adds)
        ]
        states = [shifted(value, "seq", 1) for value in sent]

    peers = lax.axis_size("head")
    rows = tokens // peers
    pieces = pl.pallas_call(
        final_kernel,
        out_shape=[jax.ShapeDtypeStruct((rows, out_weight.shape[1]), bf16)] * peers,
        scratch_shapes=[pltpu.VMEM((tokens, heads * width), bf16)],
        name="read_and_project",
    )(states[0], states[1], reads, offsets, maps, adds, norm_gain[None], out_weight)
    total = pieces[0].astype(f32)
    for turn in range(1, peers):
        total = total + rotated(pieces[turn], "head", turn).astype(f32)
    return total.astype(bf16)[None]


def solution(mesh):
    in_specs = (
        P(("parts", "rep"), "seq", "head"),
        P(("parts", "rep"), "seq", None, "head"),
        P(("parts", "rep"), "seq", None, "head"),
        P(("parts", "rep"), "seq", None, "head"),
        P(("parts", "rep"), "seq", "head"),
        P(("parts", "rep"), None),
        P(),
        P("head", None),
    )
    out_specs = P(("parts", "rep"), ("seq", "head"), None)
    return jax.shard_map(body, mesh=mesh, in_specs=in_specs, out_specs=out_specs, check_vma=False)
```

```python
import jax
import jax.numpy as jnp
from jax import lax
from jax.experimental import pallas as pl
from jax.experimental.pallas import tpu as pltpu
from jax.sharding import PartitionSpec as P

BLOCK = 64
MOST_LEN = 2048
HEADS_PER_STEP = 2
epsilon = 1e-06
f32 = jnp.float32
bf16 = jnp.bfloat16


def dot_nn(left, right):
    return lax.dot_general(left, right, (((1,), (0,)), ((), ())), preferred_element_type=f32)


def dot_nt(left, right):
    return lax.dot_general(left, right, (((1,), (1,)), ((), ())), preferred_element_type=f32)


def dot_tn(left, right):
    return lax.dot_general(left, right, (((0,), (0,)), ((), ())), preferred_element_type=f32)


def halves(value):
    top = value.astype(bf16)
    return top, (value - top.astype(f32)).astype(bf16)


def square_product(left, right):
    width = right[0].shape[1]
    side = jnp.concatenate([right[0], right[1]], axis=1)
    both = dot_nn(
        jnp.concatenate([left[0], left[1]], axis=1), jnp.concatenate([side, side], axis=0)
    )
    return both[:, :width] + both[:, width:]


def iota(shape, dim):
    return lax.broadcasted_iota(jnp.int32, shape, dim)


def local_kernel(
    lengths, query, keys, values, beta, decay, reads, offsets, maps, adds, *rest
):
    sends = rest[:-3]
    inner_mask, read_mask, edge_mask = rest[-3:]
    turn = pl.program_id(0)
    tokens = query.shape[1]
    heads_here = reads.shape[0]
    width = reads.shape[2]
    refl = keys.shape[2]
    steps = BLOCK * refl
    blocks = tokens // BLOCK
    first = lax.axis_index("seq") * tokens
    place = lax.rem(lax.axis_index("seq"), len(sends))
    row = iota((steps, steps), 0)
    col = iota((steps, steps), 1)
    eye = row == col
    unit = jnp.where(eye, 1.0, 0.0).astype(f32)
    step_col = iota((steps, 1), 0)
    token_col = step_col // refl
    refl_col = step_col % refl
    token_lane = iota((steps, BLOCK), 1)
    token_row = iota((1, steps), 1) // refl
    read_col = iota((BLOCK, 1), 0)
    read_lane = iota((BLOCK, BLOCK), 1)
    read_step = iota((BLOCK, steps), 1)
    read_token = read_step // refl
    hidden = -1e30

    @pl.when(turn == 0)
    def _():
        ends, end = [], jnp.int32(0)
        for doc in range(lengths.shape[1]):
            end = end + lengths[0, doc]
            ends.append(end)

        def start_of(position):
            start = jnp.zeros_like(position)
            for end in ends:
                start = jnp.where(end <= position, end, start)
            return start

        for block in range(blocks):
            begin = first + block * BLOCK
            start = start_of(begin + token_col)
            inner_mask[block] = jnp.where(
                (col < row) & (begin + col // refl >= start), 0.0, hidden
            )
            read_start = start_of(begin + read_col)
            read_mask[block] = jnp.where(
                (read_token <= read_col) & (begin + read_token >= read_start), 0.0, hidden
            )
            start_row = start_of(begin + token_row)
            last_start = start_of(begin + token_row * 0 + (BLOCK - 1))
            edge_mask[block, 0:1, :] = jnp.where(start_row < begin, 0.0, hidden)
            edge_mask[block, 1:2, :] = jnp.where(begin + token_row >= last_start, 0.0, hidden)

    def to_row(column):
        return jnp.sum(jnp.where(eye, column, 0.0), axis=0, keepdims=True)

    def to_col(line):
        return jnp.sum(jnp.where(eye, line, 0.0), axis=1, keepdims=True)

    chains = []
    for local in range(heads_here):
        head = turn * heads_here + local
        lanes = slice(local * width, (local + 1) * width)
        key_all = keys[0, :, :, lanes].reshape(tokens * refl, width)
        gate_all = decay[pl.ds(head, 1), :]
        beta_all = [beta[j, pl.ds(head, 1), :] for j in range(refl)]
        for block in range(blocks):
            at = block * BLOCK
            key = key_all[at * refl : at * refl + steps]
            gate = gate_all[:, at : at + BLOCK]
            cum = jnp.sum(jnp.where(token_lane <= token_col, gate, 0.0), axis=1, keepdims=True)
            beta_here = beta_all[refl - 1][:, at : at + BLOCK]
            for j in range(refl - 1):
                beta_here = jnp.where(refl_col == j, beta_all[j][:, at : at + BLOCK], beta_here)
            strength = jnp.sum(
                jnp.where(token_lane == token_col, beta_here, 0.0), axis=1, keepdims=True
            )
            gram = dot_nt(key, key)
            diagonal = jnp.where(eye, gram, 0.0)
            scale = lax.rsqrt(jnp.sum(diagonal, axis=1, keepdims=True) + epsilon)
            scale_row = lax.rsqrt(jnp.sum(diagonal, axis=0, keepdims=True) + epsilon)
            cum_row = to_row(cum)
            ratio = jnp.exp(jnp.minimum(cum - cum_row, inner_mask[block]))
            system = (strength * scale) * ratio * gram * scale_row
            chains.append(
                dict(
                    local=local,
                    block=block,
                    lanes=lanes,
                    key=key,
                    gate=gate,
                    cum_row=cum_row,
                    strength=strength,
                    scale_row=scale_row,
                    system=halves(system),
                    inverse=unit - jnp.where((row ^ col) == 1, system, 0.0),
                )
            )
    size = 2
    while size < steps:
        mask = ((row // size) ^ (col // size)) == 1
        for c in chains:
            inverse = halves(c["inverse"])
            corner = tuple(jnp.where(mask, part, jnp.zeros_like(part)) for part in c["system"])
            moved = square_product(corner, inverse)
            c["inverse"] = c["inverse"] - square_product(inverse, halves(moved))
        size *= 2
    totals = [None] * heads_here
    for c in chains:
        local, block, key = c["local"], c["block"], c["key"]
        at = block * BLOCK
        value = values[0, at : at + BLOCK, :, c["lanes"]].reshape(steps, width)
        strength_row = to_row(c["strength"])
        cum_row, scale_row = c["cum_row"], c["scale_row"]
        carry_row = jnp.exp(jnp.minimum(cum_row, edge_mask[block, 0:1, :]))
        value_side = jnp.concatenate(halves(c["inverse"] * strength_row), axis=1)
        key_side = jnp.concatenate(
            halves(c["inverse"] * (strength_row * carry_row * scale_row)), axis=1
        )
        writes = jnp.concatenate(
            [
                dot_nn(value_side, jnp.concatenate([value, value], axis=0)),
                dot_nn(key_side, jnp.concatenate([key, key], axis=0)),
            ],
            axis=1,
        )
        fade_row = scale_row * jnp.exp(
            jnp.minimum(cum_row[:, steps - 1 :] - cum_row, edge_mask[block, 1:2, :])
        )
        faded = jnp.concatenate(halves(to_col(fade_row) * writes), axis=0)
        summed = dot_tn(jnp.concatenate([key, key], axis=0), faded)
        block_add = summed[:, :width]
        block_map = carry_row[:, steps - 1 :] * unit - summed[:, width:]
        query_here = query[0, at : at + BLOCK, c["lanes"]]
        query_f = query_here.astype(f32)
        query_scale = lax.rsqrt(
            jnp.sum(query_f * query_f, axis=1, keepdims=True) + epsilon
        ) * (width ** (-0.5))
        read_cum = jnp.sum(
            jnp.where(read_lane <= read_col, c["gate"], 0.0), axis=1, keepdims=True
        )
        weights = jnp.exp(jnp.minimum(read_cum - cum_row, read_mask[block]))
        weights = weights * dot_nt(query_here, key) * query_scale * scale_row
        writes_top = writes.astype(bf16)
        seen = dot_nn(
            jnp.concatenate(halves(weights), axis=1),
            jnp.concatenate([writes_top, writes_top], axis=0),
        )
        read_carry = jnp.sum(
            jnp.where(read_step == read_col * refl, carry_row, 0.0), axis=1, keepdims=True
        )
        offsets[local, at : at + BLOCK, :] = seen[:, :width]
        reads[local, at : at + BLOCK, :] = (
            (read_carry * query_scale) * query_f - seen[:, width:]
        ).astype(bf16)
        maps[local, block] = block_map.astype(bf16)
        adds[local, block] = block_add
        if totals[local] is None:
            totals[local] = jnp.concatenate([block_map, block_add], axis=1)
        else:
            top, low = halves(block_map)
            tall = jnp.concatenate(
                [
                    jnp.concatenate([top, top], axis=1),
                    jnp.concatenate([low, jnp.zeros_like(low)], axis=1),
                ],
                axis=0,
            )
            joined = dot_nn(tall, jnp.concatenate(halves(totals[local]), axis=0))
            joined = joined[:width] + joined[width:]
            totals[local] = jnp.concatenate(
                [joined[:, :width], joined[:, width:] + block_add], axis=1
            )
    for local in range(heads_here):
        both = totals[local].astype(bf16)
        slot = (turn * heads_here + local) ^ place
        for other, send in enumerate(sends):

            @pl.when(slot == other)
            def _():
                send[...] = both


def chosen(index, options):
    value = options[0]
    for other in range(1, len(options)):
        value = jnp.where(index == other, options[other], value)
    return value


def run_states(place, parts, state):
    states = []
    width = parts[0].shape[0]
    for member in range(len(parts)):
        states.append(state)
        both = chosen(place ^ member, [part[...] for part in parts])
        top = both[:, :width]
        added = both[:, width:].astype(f32)
        if state is None:
            state = added
        else:
            state = added + dot_nn(
                jnp.concatenate([top, top], axis=1), jnp.concatenate(halves(state), axis=0)
            )
    return states, state


def macro_kernel(*refs):
    count = len(refs) - 1
    place = lax.rem(lax.axis_index("seq"), count)
    states, state = run_states(place, refs[:count], None)
    refs[-1][...] = state.astype(bf16)


def hop_kernel(arrived, *refs):
    count = len(refs) - 1
    place = lax.rem(lax.axis_index("seq"), count)
    states, state = run_states(place, refs[:count], arrived[...].astype(f32))
    refs[-1][...] = state.astype(bf16)


def spread_kernel(arrived, *refs):
    count = len(refs) // 2
    place = lax.rem(lax.axis_index("seq"), count)
    states, state = run_states(place, refs[:count], arrived[...].astype(f32))
    states = [value.astype(bf16) for value in states]
    for turn in range(count):
        refs[count + turn][...] = chosen(place ^ turn, states)


def final_kernel(*refs):
    heads = refs[-1].shape[1] // refs[0].shape[1]
    first_states = refs[:heads]
    reads, offsets, maps, adds, gain, weight = refs[heads : heads + 6]
    outs, normed = refs[heads + 6 : -1], refs[-1]
    heads, tokens, width = reads.shape
    blocks = tokens // BLOCK
    place = lax.rem(lax.axis_index("seq"), heads)
    held = [ref[...] for ref in first_states]
    states = [chosen(place ^ head, held) for head in range(heads)]
    for block in range(blocks):
        at = block * BLOCK
        for head in range(heads):
            state = states[head]
            out = dot_nn(reads[head, at : at + BLOCK, :], state) + offsets[head, at : at + BLOCK, :]
            out = out * lax.rsqrt(jnp.mean(out * out, axis=1, keepdims=True) + epsilon)
            normed[at : at + BLOCK, head * width : (head + 1) * width] = (
                out * gain[...]
            ).astype(bf16)
            if block + 1 < blocks:
                states[head] = (dot_nn(maps[head, block], state) + adds[head, block]).astype(bf16)
    peers = len(outs)
    rows = tokens // peers
    me = lax.axis_index("head")
    for turn in range(peers):
        chunk = me ^ turn
        here = normed[pl.ds(pl.multiple_of(chunk * rows, rows), rows), :]
        outs[turn][...] = dot_nn(here, weight[...]).astype(bf16)


def exchanged(value, axis, mask):
    count = lax.axis_size(axis)
    return lax.ppermute(value, axis, [(source, source ^ mask) for source in range(count)])


def rotated(value, axis, steps):
    count = lax.axis_size(axis)
    return lax.ppermute(value, axis, [(source, (source + steps) % count) for source in range(count)])


def grant(mebibytes):
    return pltpu.CompilerParams(vmem_limit_bytes=mebibytes << 20)


def body(
    queries,
    reflect_keys,
    reflect_values,
    reflect_beta,
    log_decay,
    prompt_lengths,
    norm_gain,
    out_weight,
):
    tokens = queries.shape[1]
    refl = reflect_keys.shape[2]
    heads = reflect_beta.shape[3]
    width = queries.shape[2] // heads
    blocks = tokens // BLOCK
    steps = refl * BLOCK
    beta = reflect_beta[0].transpose(1, 2, 0)
    decay = log_decay[0].transpose(1, 0)
    pair = HEADS_PER_STEP
    rows_spec = pl.BlockSpec((pair, tokens, width), lambda h: (h, 0, 0))
    square_spec = pl.BlockSpec((pair, blocks, width, width), lambda h: (h, 0, 0, 0))
    send_spec = pl.BlockSpec((width, 2 * width), lambda h: (0, 0))
    both_shape = jax.ShapeDtypeStruct((width, 2 * width), bf16)
    reads, offsets, maps, adds, *mine = pl.pallas_call(
        local_kernel,
        grid=(heads // pair,),
        in_specs=[
            pl.BlockSpec(memory_space=pltpu.SMEM),
            pl.BlockSpec((1, tokens, pair * width), lambda h: (0, 0, h)),
            pl.BlockSpec((1, tokens, refl, pair * width), lambda h: (0, 0, 0, h)),
            pl.BlockSpec((1, tokens, refl, pair * width), lambda h: (0, 0, 0, h)),
            pl.BlockSpec((refl, heads, tokens), lambda h: (0, 0, 0)),
            pl.BlockSpec((heads, tokens), lambda h: (0, 0)),
        ],
        out_specs=[rows_spec, rows_spec, square_spec, square_spec] + [send_spec] * heads,
        out_shape=[
            jax.ShapeDtypeStruct((heads, tokens, width), bf16),
            jax.ShapeDtypeStruct((heads, tokens, width), f32),
            jax.ShapeDtypeStruct((heads, blocks, width, width), bf16),
            jax.ShapeDtypeStruct((heads, blocks, width, width), f32),
        ]
        + [both_shape] * heads,
        scratch_shapes=[
            pltpu.VMEM((blocks, steps, steps), f32),
            pltpu.VMEM((blocks, BLOCK, steps), f32),
            pltpu.VMEM((blocks, 8, steps), f32),
        ],
        compiler_params=grant(20),
        name="local_blocks",
    )(prompt_lengths, queries, reflect_keys, reflect_values, beta, decay)

    state_shape = jax.ShapeDtypeStruct((width, width), bf16)
    parts = [mine[0]] + [exchanged(mine[r], "seq", r) for r in range(1, heads)]
    sent = pl.pallas_call(
        macro_kernel, out_shape=state_shape, compiler_params=grant(4), name="macro"
    )(*parts)
    macro_hops = -(-(MOST_LEN - 1) // (tokens * heads))
    arrived = rotated(sent, "seq", heads)
    for hop in range(macro_hops - 1):
        sent = pl.pallas_call(
            hop_kernel, out_shape=state_shape, compiler_params=grant(4), name="hop"
        )(arrived, *parts)
        arrived = rotated(sent, "seq", heads)
    given = pl.pallas_call(
        spread_kernel, out_shape=[state_shape] * heads, compiler_params=grant(4), name="spread"
    )(arrived, *parts)
    states = [given[0]] + [exchanged(given[r], "seq", r) for r in range(1, heads)]

    peers = lax.axis_size("head")
    rows = tokens // peers
    pieces = pl.pallas_call(
        final_kernel,
        out_shape=[jax.ShapeDtypeStruct((rows, out_weight.shape[1]), bf16)] * peers,
        scratch_shapes=[pltpu.VMEM((tokens, heads * width), bf16)],
        compiler_params=grant(16),
        name="read_and_project",
    )(*states, reads, offsets, maps, adds, norm_gain[None], out_weight)
    total = pieces[0].astype(f32)
    for turn in range(1, peers):
        total = total + exchanged(pieces[turn], "head", turn).astype(f32)
    return total.astype(bf16)[None]


def solution(mesh):
    in_specs = (
        P(("parts", "rep"), "seq", "head"),
        P(("parts", "rep"), "seq", None, "head"),
        P(("parts", "rep"), "seq", None, "head"),
        P(("parts", "rep"), "seq", None, "head"),
        P(("parts", "rep"), "seq", "head"),
        P(("parts", "rep"), None),
        P(),
        P("head", None),
    )
    out_specs = P(("parts", "rep"), ("seq", "head"), None)
    return jax.shard_map(body, mesh=mesh, in_specs=in_specs, out_specs=out_specs, check_vma=False)
```

```python
import jax
import jax.numpy as jnp
from jax import lax
from jax.experimental import pallas as pl
from jax.experimental.pallas import tpu as pltpu
from jax.sharding import PartitionSpec as P

BLOCK = 64
MOST_LEN = 2048
HEADS_PER_STEP = 2
epsilon = 1e-06
f32 = jnp.float32
bf16 = jnp.bfloat16


def dot_nn(left, right):
    return lax.dot_general(left, right, (((1,), (0,)), ((), ())), preferred_element_type=f32)


def dot_nt(left, right):
    return lax.dot_general(left, right, (((1,), (1,)), ((), ())), preferred_element_type=f32)


def dot_tn(left, right):
    return lax.dot_general(left, right, (((0,), (0,)), ((), ())), preferred_element_type=f32)


def halves(value):
    top = value.astype(bf16)
    return top, (value - top.astype(f32)).astype(bf16)


def square_product(left, right):
    width = right[0].shape[1]
    side = jnp.concatenate([right[0], right[1]], axis=1)
    both = dot_nn(
        jnp.concatenate([left[0], left[1]], axis=1), jnp.concatenate([side, side], axis=0)
    )
    return both[:, :width] + both[:, width:]


def iota(shape, dim):
    return lax.broadcasted_iota(jnp.int32, shape, dim)


def local_kernel(
    far_lengths, far_query, far_keys, far_values, far_beta, far_decay, far_weight, far_gain, reads, offsets, maps, adds, *rest
):
    weight, gain = rest[:2]
    sends = rest[2:-10]
    inner_mask, read_mask, edge_mask = rest[-10:-7]
    lengths, query_all, keys_all, values_all, beta, decay, done = rest[-7:]
    turn = pl.program_id(0)
    turns = query_all.shape[0]
    tokens = query_all.shape[1]
    heads_here = reads.shape[0]
    width = reads.shape[2]
    refl = keys_all.shape[2]
    steps = BLOCK * refl
    blocks = tokens // BLOCK
    first = lax.axis_index("seq") * tokens
    place = lax.rem(lax.axis_index("seq"), len(sends))
    row = iota((steps, steps), 0)
    col = iota((steps, steps), 1)
    eye = row == col
    unit = jnp.where(eye, 1.0, 0.0).astype(f32)
    step_col = iota((steps, 1), 0)
    token_col = step_col // refl
    refl_col = step_col % refl
    token_lane = iota((steps, BLOCK), 1)
    token_row = iota((1, steps), 1) // refl
    read_col = iota((BLOCK, 1), 0)
    read_lane = iota((BLOCK, BLOCK), 1)
    read_step = iota((BLOCK, steps), 1)
    read_token = read_step // refl
    hidden = -1e30

    span = heads_here * width
    copies = [
        pltpu.make_async_copy(source, target, done.at[index])
        for index, (source, target) in enumerate(
            [(far_lengths, lengths), (far_decay, decay), (far_beta, beta)]
        )
    ]

    passed = [
        pltpu.make_async_copy(source, target, done.at[3 + 3 * turns + index])
        for index, (source, target) in enumerate([(far_weight, weight), (far_gain, gain)])
    ]

    def fetch(kind, part):
        lanes = pl.ds(part * span, span)
        source, target = [
            (far_keys.at[0, :, :, lanes], keys_all.at[part]),
            (far_values.at[0, :, :, lanes], values_all.at[part]),
            (far_query.at[0, :, lanes], query_all.at[part]),
        ][kind]
        return pltpu.make_async_copy(source, target, done.at[3 + kind * turns + part])

    @pl.when(turn == 0)
    def _():
        for copy in copies:
            copy.start()
        for part in range(turns):
            for kind in range(3):
                fetch(kind, part).start()
        for copy in passed:
            copy.start()
        for copy in copies:
            copy.wait()
        ends, end = [], jnp.int32(0)
        for doc in range(lengths.shape[1]):
            end = end + lengths[0, doc]
            ends.append(end)

        def start_of(position):
            start = jnp.zeros_like(position)
            for end in ends:
                start = jnp.where(end <= position, end, start)
            return start

        for block in range(blocks):
            begin = first + block * BLOCK
            start = start_of(begin + token_col)
            inner_mask[block] = jnp.where(
                (col < row) & (begin + col // refl >= start), 0.0, hidden
            )
            read_start = start_of(begin + read_col)
            read_mask[block] = jnp.where(
                (read_token <= read_col) & (begin + read_token >= read_start), 0.0, hidden
            )
            start_row = start_of(begin + token_row)
            last_start = start_of(begin + token_row * 0 + (BLOCK - 1))
            edge_mask[block, 0:1, :] = jnp.where(start_row < begin, 0.0, hidden)
            edge_mask[block, 1:2, :] = jnp.where(begin + token_row >= last_start, 0.0, hidden)

    def to_row(column):
        return jnp.sum(jnp.where(eye, column, 0.0), axis=0, keepdims=True)

    def to_col(line):
        return jnp.sum(jnp.where(eye, line, 0.0), axis=1, keepdims=True)

    keys, values, query = keys_all.at[turn], values_all.at[turn], query_all.at[turn]
    for kind in range(3):
        fetch(kind, turn).wait()
    chains = []
    for local in range(heads_here):
        head = turn * heads_here + local
        lanes = slice(local * width, (local + 1) * width)
        key_all = keys[:, :, lanes].reshape(tokens * refl, width)
        gate_all = decay[pl.ds(head, 1), :]
        beta_all = [beta[j, pl.ds(head, 1), :] for j in range(refl)]
        for block in range(blocks):
            at = block * BLOCK
            key = key_all[at * refl : at * refl + steps]
            gate = gate_all[:, at : at + BLOCK]
            cum = jnp.sum(jnp.where(token_lane <= token_col, gate, 0.0), axis=1, keepdims=True)
            beta_here = beta_all[refl - 1][:, at : at + BLOCK]
            for j in range(refl - 1):
                beta_here = jnp.where(refl_col == j, beta_all[j][:, at : at + BLOCK], beta_here)
            strength = jnp.sum(
                jnp.where(token_lane == token_col, beta_here, 0.0), axis=1, keepdims=True
            )
            gram = dot_nt(key, key)
            diagonal = jnp.where(eye, gram, 0.0)
            scale = lax.rsqrt(jnp.sum(diagonal, axis=1, keepdims=True) + epsilon)
            scale_row = lax.rsqrt(jnp.sum(diagonal, axis=0, keepdims=True) + epsilon)
            cum_row = to_row(cum)
            ratio = jnp.exp(jnp.minimum(cum - cum_row, inner_mask[block]))
            system = (strength * scale) * ratio * gram * scale_row
            chains.append(
                dict(
                    local=local,
                    block=block,
                    lanes=lanes,
                    key=key,
                    gate=gate,
                    cum_row=cum_row,
                    strength=strength,
                    scale_row=scale_row,
                    system=halves(system),
                    inverse=unit - jnp.where((row ^ col) == 1, system, 0.0),
                )
            )
    size = 2
    while size < steps:
        mask = ((row // size) ^ (col // size)) == 1
        for c in chains:
            inverse = halves(c["inverse"])
            corner = tuple(jnp.where(mask, part, jnp.zeros_like(part)) for part in c["system"])
            moved = square_product(corner, inverse)
            c["inverse"] = c["inverse"] - square_product(inverse, halves(moved))
        size *= 2
    totals = [None] * heads_here
    for c in chains:
        local, block, key = c["local"], c["block"], c["key"]
        at = block * BLOCK
        value = values[at : at + BLOCK, :, c["lanes"]].reshape(steps, width)
        strength_row = to_row(c["strength"])
        cum_row, scale_row = c["cum_row"], c["scale_row"]
        carry_row = jnp.exp(jnp.minimum(cum_row, edge_mask[block, 0:1, :]))
        value_side = jnp.concatenate(halves(c["inverse"] * strength_row), axis=1)
        key_side = jnp.concatenate(
            halves(c["inverse"] * (strength_row * carry_row * scale_row)), axis=1
        )
        writes = jnp.concatenate(
            [
                dot_nn(value_side, jnp.concatenate([value, value], axis=0)),
                dot_nn(key_side, jnp.concatenate([key, key], axis=0)),
            ],
            axis=1,
        )
        fade_row = scale_row * jnp.exp(
            jnp.minimum(cum_row[:, steps - 1 :] - cum_row, edge_mask[block, 1:2, :])
        )
        faded = jnp.concatenate(halves(to_col(fade_row) * writes), axis=0)
        summed = dot_tn(jnp.concatenate([key, key], axis=0), faded)
        block_add = summed[:, :width]
        block_map = carry_row[:, steps - 1 :] * unit - summed[:, width:]
        query_here = query[at : at + BLOCK, c["lanes"]]
        query_f = query_here.astype(f32)
        query_scale = lax.rsqrt(
            jnp.sum(query_f * query_f, axis=1, keepdims=True) + epsilon
        ) * (width ** (-0.5))
        read_cum = jnp.sum(
            jnp.where(read_lane <= read_col, c["gate"], 0.0), axis=1, keepdims=True
        )
        weights = jnp.exp(jnp.minimum(read_cum - cum_row, read_mask[block]))
        weights = weights * dot_nt(query_here, key) * query_scale * scale_row
        writes_top = writes.astype(bf16)
        seen = dot_nn(
            jnp.concatenate(halves(weights), axis=1),
            jnp.concatenate([writes_top, writes_top], axis=0),
        )
        read_carry = jnp.sum(
            jnp.where(read_step == read_col * refl, carry_row, 0.0), axis=1, keepdims=True
        )
        offsets[local, at : at + BLOCK, :] = seen[:, :width]
        reads[local, at : at + BLOCK, :] = (
            (read_carry * query_scale) * query_f - seen[:, width:]
        ).astype(bf16)
        maps[local, block] = block_map.astype(bf16)
        adds[local, block] = block_add
        if totals[local] is None:
            totals[local] = jnp.concatenate([block_map, block_add], axis=1)
        else:
            top, low = halves(block_map)
            tall = jnp.concatenate(
                [
                    jnp.concatenate([top, top], axis=1),
                    jnp.concatenate([low, jnp.zeros_like(low)], axis=1),
                ],
                axis=0,
            )
            joined = dot_nn(tall, jnp.concatenate(halves(totals[local]), axis=0))
            joined = joined[:width] + joined[width:]
            totals[local] = jnp.concatenate(
                [joined[:, :width], joined[:, width:] + block_add], axis=1
            )
    for local in range(heads_here):
        both = totals[local].astype(bf16)
        slot = (turn * heads_here + local) ^ place
        for other, send in enumerate(sends):

            @pl.when(slot == other)
            def _():
                send[...] = both

    @pl.when(turn == turns - 1)
    def _():
        for copy in passed:
            copy.wait()


def chosen(index, options):
    value = options[0]
    for other in range(1, len(options)):
        value = jnp.where(index == other, options[other], value)
    return value


def run_states(place, parts, state):
    states = []
    width = parts[0].shape[0]
    for member in range(len(parts)):
        states.append(state)
        both = chosen(place ^ member, [part[...] for part in parts])
        top = both[:, :width]
        added = both[:, width:].astype(f32)
        if state is None:
            state = added
        else:
            state = added + dot_nn(
                jnp.concatenate([top, top], axis=1), jnp.concatenate(halves(state), axis=0)
            )
    return states, state


def macro_kernel(*refs):
    count = len(refs) - 1
    place = lax.rem(lax.axis_index("seq"), count)
    states, state = run_states(place, refs[:count], None)
    refs[-1][...] = state.astype(bf16)


def hop_kernel(arrived, *refs):
    count = len(refs) - 1
    place = lax.rem(lax.axis_index("seq"), count)
    states, state = run_states(place, refs[:count], arrived[...].astype(f32))
    refs[-1][...] = state.astype(bf16)


def spread_kernel(arrived, *refs):
    count = len(refs) // 2
    place = lax.rem(lax.axis_index("seq"), count)
    states, state = run_states(place, refs[:count], arrived[...].astype(f32))
    states = [value.astype(bf16) for value in states]
    for turn in range(count):
        refs[count + turn][...] = chosen(place ^ turn, states)


def final_kernel(*refs):
    heads = refs[-1].shape[1] // refs[0].shape[1]
    first_states = refs[:heads]
    reads, offsets, maps, adds, gain, weight = refs[heads : heads + 6]
    outs, normed = refs[heads + 6 : -1], refs[-1]
    heads, tokens, width = reads.shape
    blocks = tokens // BLOCK
    place = lax.rem(lax.axis_index("seq"), heads)
    held = [ref[...] for ref in first_states]
    states = [chosen(place ^ head, held) for head in range(heads)]
    for block in range(blocks):
        at = block * BLOCK
        for head in range(heads):
            state = states[head]
            out = dot_nn(reads[head, at : at + BLOCK, :], state) + offsets[head, at : at + BLOCK, :]
            out = out * lax.rsqrt(jnp.mean(out * out, axis=1, keepdims=True) + epsilon)
            normed[at : at + BLOCK, head * width : (head + 1) * width] = (
                out * gain[...]
            ).astype(bf16)
            if block + 1 < blocks:
                states[head] = (dot_nn(maps[head, block], state) + adds[head, block]).astype(bf16)
    peers = len(outs)
    rows = tokens // peers
    me = lax.axis_index("head")
    for turn in range(peers):
        chunk = me ^ turn
        here = normed[pl.ds(pl.multiple_of(chunk * rows, rows), rows), :]
        outs[turn][...] = dot_nn(here, weight[...]).astype(bf16)


def exchanged(value, axis, mask):
    count = lax.axis_size(axis)
    return lax.ppermute(value, axis, [(source, source ^ mask) for source in range(count)])


def shifted(value, axis, steps):
    count = lax.axis_size(axis)
    return lax.ppermute(value, axis, [(source, source + steps) for source in range(count - steps)])


def grant(mebibytes):
    return pltpu.CompilerParams(vmem_limit_bytes=mebibytes << 20)


def body(
    queries,
    reflect_keys,
    reflect_values,
    reflect_beta,
    log_decay,
    prompt_lengths,
    norm_gain,
    out_weight,
):
    tokens = queries.shape[1]
    refl = reflect_keys.shape[2]
    heads = reflect_beta.shape[3]
    width = queries.shape[2] // heads
    blocks = tokens // BLOCK
    steps = refl * BLOCK
    beta = reflect_beta[0].transpose(1, 2, 0)
    decay = log_decay[0].transpose(1, 0)
    pair = HEADS_PER_STEP
    rows_spec = pl.BlockSpec((pair, tokens, width), lambda h: (h, 0, 0))
    square_spec = pl.BlockSpec((pair, blocks, width, width), lambda h: (h, 0, 0, 0))
    send_spec = pl.BlockSpec((width, 2 * width), lambda h: (0, 0))
    both_shape = jax.ShapeDtypeStruct((width, 2 * width), bf16)
    reads, offsets, maps, adds, weight, gain, *mine = pl.pallas_call(
        local_kernel,
        grid=(heads // pair,),
        in_specs=[pl.BlockSpec(memory_space=pltpu.HBM)] * 8,
        out_specs=[rows_spec, rows_spec, square_spec, square_spec]
        + [pl.BlockSpec(memory_space=pl.ANY)] * 2
        + [send_spec] * heads,
        out_shape=[
            jax.ShapeDtypeStruct((heads, tokens, width), bf16),
            jax.ShapeDtypeStruct((heads, tokens, width), f32),
            jax.ShapeDtypeStruct((heads, blocks, width, width), bf16),
            jax.ShapeDtypeStruct((heads, blocks, width, width), f32),
            jax.ShapeDtypeStruct(out_weight.shape, bf16),
            jax.ShapeDtypeStruct((1, width), f32),
        ]
        + [both_shape] * heads,
        scratch_shapes=[
            pltpu.VMEM((blocks, steps, steps), f32),
            pltpu.VMEM((blocks, BLOCK, steps), f32),
            pltpu.VMEM((blocks, 8, steps), f32),
            pltpu.SMEM(prompt_lengths.shape, jnp.int32),
            pltpu.VMEM((heads // pair, tokens, pair * width), bf16),
            pltpu.VMEM((heads // pair, tokens, refl, pair * width), bf16),
            pltpu.VMEM((heads // pair, tokens, refl, pair * width), bf16),
            pltpu.VMEM(beta.shape, f32),
            pltpu.VMEM(decay.shape, f32),
            pltpu.SemaphoreType.DMA((5 + 3 * (heads // pair),)),
        ],
        compiler_params=grant(20),
        name="local_blocks",
    )(
        *[
            pltpu.with_memory_space_constraint(array, pltpu.HBM)
            for array in (prompt_lengths, queries, reflect_keys, reflect_values, beta, decay)
            + (out_weight, norm_gain[None])
        ]
    )

    state_shape = jax.ShapeDtypeStruct((width, width), bf16)
    parts = [mine[0]] + [exchanged(mine[r], "seq", r) for r in range(1, heads)]
    sent = pl.pallas_call(
        macro_kernel, out_shape=state_shape, compiler_params=grant(4), name="macro"
    )(*parts)
    macro_hops = -(-(MOST_LEN - 1) // (tokens * heads))
    arrived = shifted(sent, "seq", heads)
    for hop in range(macro_hops - 1):
        sent = pl.pallas_call(
            hop_kernel, out_shape=state_shape, compiler_params=grant(4), name="hop"
        )(arrived, *parts)
        arrived = shifted(sent, "seq", heads)
    given = pl.pallas_call(
        spread_kernel, out_shape=[state_shape] * heads, compiler_params=grant(4), name="spread"
    )(arrived, *parts)
    states = [given[0]] + [exchanged(given[r], "seq", r) for r in range(1, heads)]

    peers = lax.axis_size("head")
    rows = tokens // peers
    pieces = pl.pallas_call(
        final_kernel,
        out_shape=[jax.ShapeDtypeStruct((rows, out_weight.shape[1]), bf16)] * peers,
        scratch_shapes=[pltpu.VMEM((tokens, heads * width), bf16)],
        compiler_params=grant(16),
        name="read_and_project",
    )(*states, reads, offsets, maps, adds, gain, weight)
    total = pieces[0].astype(f32)
    for turn in (2, 1, 3):
        total = total + exchanged(pieces[turn], "head", turn).astype(f32)
    return total.astype(bf16)[None]


def solution(mesh):
    in_specs = (
        P(("parts", "rep"), "seq", "head"),
        P(("parts", "rep"), "seq", None, "head"),
        P(("parts", "rep"), "seq", None, "head"),
        P(("parts", "rep"), "seq", None, "head"),
        P(("parts", "rep"), "seq", "head"),
        P(("parts", "rep"), None),
        P(),
        P("head", None),
    )
    out_specs = P(("parts", "rep"), ("seq", "head"), None)
    return jax.shard_map(body, mesh=mesh, in_specs=in_specs, out_specs=out_specs, check_vma=False)
```

```python
import functools

import jax
import jax.numpy as jnp
from jax import lax
from jax.experimental import pallas as pl
from jax.experimental.pallas import tpu as pltpu
from jax.sharding import PartitionSpec as P

BLOCK = 64
MOST_LEN = 2048
HEADS_PER_STEP = 2
epsilon = 1e-06
f32 = jnp.float32
bf16 = jnp.bfloat16


def dot_nn(left, right):
    return lax.dot_general(left, right, (((1,), (0,)), ((), ())), preferred_element_type=f32)


def dot_nt(left, right):
    return lax.dot_general(left, right, (((1,), (1,)), ((), ())), preferred_element_type=f32)


def dot_tn(left, right):
    return lax.dot_general(left, right, (((0,), (0,)), ((), ())), preferred_element_type=f32)


def halves(value):
    top = value.astype(bf16)
    return top, (value - top.astype(f32)).astype(bf16)


def square_product(left, right):
    width = right[0].shape[1]
    side = jnp.concatenate([right[0], right[1]], axis=1)
    both = dot_nn(
        jnp.concatenate([left[0], left[1]], axis=1), jnp.concatenate([side, side], axis=0)
    )
    return both[:, :width] + both[:, width:]


def iota(shape, dim):
    return lax.broadcasted_iota(jnp.int32, shape, dim)


def local_kernel(
    far_lengths, far_query, far_keys, far_values, far_beta, far_decay, far_weight, far_gain, reads, offsets, maps, adds, *rest
):
    weight, gain = rest[:2]
    sends = rest[2:-10]
    inner_mask, read_mask, edge_mask = rest[-10:-7]
    lengths, query_all, keys_all, values_all, beta, decay, done = rest[-7:]
    turn = pl.program_id(0)
    turns = query_all.shape[0]
    tokens = query_all.shape[1]
    heads_here = reads.shape[0]
    width = reads.shape[2]
    refl = keys_all.shape[2]
    steps = BLOCK * refl
    blocks = tokens // BLOCK
    first = lax.axis_index("seq") * tokens
    place = lax.rem(lax.axis_index("seq"), len(sends))
    row = iota((steps, steps), 0)
    col = iota((steps, steps), 1)
    eye = row == col
    unit = jnp.where(eye, 1.0, 0.0).astype(f32)
    step_col = iota((steps, 1), 0)
    token_col = step_col // refl
    refl_col = step_col % refl
    token_lane = iota((steps, BLOCK), 1)
    token_row = iota((1, steps), 1) // refl
    read_col = iota((BLOCK, 1), 0)
    read_lane = iota((BLOCK, BLOCK), 1)
    read_step = iota((BLOCK, steps), 1)
    read_token = read_step // refl
    hidden = -1e30

    span = heads_here * width
    copies = [
        pltpu.make_async_copy(source, target, done.at[index])
        for index, (source, target) in enumerate(
            [(far_lengths, lengths), (far_decay, decay), (far_beta, beta)]
        )
    ]

    passed = [
        pltpu.make_async_copy(source, target, done.at[3 + 3 * turns + index])
        for index, (source, target) in enumerate([(far_weight, weight), (far_gain, gain)])
    ]

    def fetch(kind, part):
        lanes = pl.ds(part * span, span)
        source, target = [
            (far_keys.at[0, :, :, lanes], keys_all.at[part]),
            (far_values.at[0, :, :, lanes], values_all.at[part]),
            (far_query.at[0, :, lanes], query_all.at[part]),
        ][kind]
        return pltpu.make_async_copy(source, target, done.at[3 + kind * turns + part])

    @pl.when(turn == 0)
    def _():
        for copy in copies:
            copy.start()
        for part in range(turns):
            for kind in range(3):
                fetch(kind, part).start()
        for copy in passed:
            copy.start()
        for copy in copies:
            copy.wait()
        ends, end = [], jnp.int32(0)
        for doc in range(lengths.shape[1]):
            end = end + lengths[0, doc]
            ends.append(end)

        def start_of(position):
            start = jnp.zeros_like(position)
            for end in ends:
                start = jnp.where(end <= position, end, start)
            return start

        for block in range(blocks):
            begin = first + block * BLOCK
            start = start_of(begin + token_col)
            inner_mask[block] = jnp.where(
                (col < row) & (begin + col // refl >= start), 0.0, hidden
            )
            read_start = start_of(begin + read_col)
            read_mask[block] = jnp.where(
                (read_token <= read_col) & (begin + read_token >= read_start), 0.0, hidden
            )
            start_row = start_of(begin + token_row)
            last_start = start_of(begin + token_row * 0 + (BLOCK - 1))
            edge_mask[block, 0:1, :] = jnp.where(start_row < begin, 0.0, hidden)
            edge_mask[block, 1:2, :] = jnp.where(begin + token_row >= last_start, 0.0, hidden)

    def to_row(column):
        return jnp.sum(jnp.where(eye, column, 0.0), axis=0, keepdims=True)

    def to_col(line):
        return jnp.sum(jnp.where(eye, line, 0.0), axis=1, keepdims=True)

    keys, values, query = keys_all.at[turn], values_all.at[turn], query_all.at[turn]
    for kind in range(3):
        fetch(kind, turn).wait()
    chains = []
    for block in range(blocks):
        for local in range(heads_here):
            lanes = slice(local * width, (local + 1) * width)
            at = block * BLOCK
            rows = slice(at, at + BLOCK)
            chains.append(
                dict(
                    local=local,
                    block=block,
                    rows=rows,
                    lanes=lanes,
                    head=turn * heads_here + local,
                    key=keys[rows, :, lanes].reshape(steps, width),
                )
            )
    for c in chains:
        c["gram"] = dot_nt(c["key"], c["key"])
    for c in chains:
        gate = decay[pl.ds(c["head"], 1), :][:, c["rows"]]
        cum = jnp.sum(jnp.where(token_lane <= token_col, gate, 0.0), axis=1, keepdims=True)
        beta_here = beta[refl - 1, pl.ds(c["head"], 1), :][:, c["rows"]]
        for j in range(refl - 1):
            beta_here = jnp.where(
                refl_col == j, beta[j, pl.ds(c["head"], 1), :][:, c["rows"]], beta_here
            )
        c["cum"] = cum
        c["strength"] = jnp.sum(
            jnp.where(token_lane == token_col, beta_here, 0.0), axis=1, keepdims=True
        )
    for c in chains:
        diagonal = jnp.where(eye, c["gram"], 0.0)
        c["scale"] = lax.rsqrt(jnp.sum(diagonal, axis=1, keepdims=True) + epsilon)
        c["scale_row"] = lax.rsqrt(jnp.sum(diagonal, axis=0, keepdims=True) + epsilon)
        c["cum_row"] = to_row(c["cum"])
        c["strength_row"] = to_row(c["strength"])
    for c in chains:
        ratio = jnp.exp(jnp.minimum(c["cum"] - c["cum_row"], inner_mask[c["block"]]))
        system = (c["strength"] * c["scale"]) * ratio * c["gram"] * c["scale_row"]
        c["system"] = halves(system)
        c["inverse"] = unit - jnp.where((row ^ col) == 1, system, 0.0)
    size = 2
    while size < steps:
        mask = ((row // size) ^ (col // size)) == 1
        for c in chains:
            c["halves"] = halves(c["inverse"])
            corner = tuple(jnp.where(mask, part, jnp.zeros_like(part)) for part in c["system"])
            c["moved"] = square_product(corner, c["halves"])
        for c in chains:
            c["inverse"] = c["inverse"] - square_product(c["halves"], halves(c["moved"]))
        size *= 2
    for c in chains:
        value = values[c["rows"], :, c["lanes"]].reshape(steps, width)
        carry_row = jnp.exp(jnp.minimum(c["cum_row"], edge_mask[c["block"], 0:1, :]))
        c["carry_row"] = carry_row
        value_side = jnp.concatenate(halves(c["inverse"] * c["strength_row"]), axis=1)
        key_side = jnp.concatenate(
            halves(c["inverse"] * (c["strength_row"] * carry_row * c["scale_row"])), axis=1
        )
        c["twice"] = jnp.concatenate([c["key"], c["key"]], axis=0)
        c["writes"] = jnp.concatenate(
            [
                dot_nn(value_side, jnp.concatenate([value, value], axis=0)),
                dot_nn(key_side, c["twice"]),
            ],
            axis=1,
        )
    for c in chains:
        cum_row = c["cum_row"]
        fade_row = c["scale_row"] * jnp.exp(
            jnp.minimum(cum_row[:, steps - 1 :] - cum_row, edge_mask[c["block"], 1:2, :])
        )
        faded = jnp.concatenate(halves(to_col(fade_row) * c["writes"]), axis=0)
        summed = dot_tn(c["twice"], faded)
        c["add"] = summed[:, :width]
        c["map"] = c["carry_row"][:, steps - 1 :] * unit - summed[:, width:]
    for c in chains:
        maps[c["local"], c["block"]] = c["map"].astype(bf16)
        adds[c["local"], c["block"]] = c["add"]
    totals = [None] * heads_here
    for c in chains:
        local, rows = c["local"], c["rows"]
        if totals[local] is None:
            totals[local] = jnp.concatenate([c["map"], c["add"]], axis=1)
        else:
            top, low = halves(c["map"])
            tall = jnp.concatenate(
                [
                    jnp.concatenate([top, top], axis=1),
                    jnp.concatenate([low, jnp.zeros_like(low)], axis=1),
                ],
                axis=0,
            )
            joined = dot_nn(tall, jnp.concatenate(halves(totals[local]), axis=0))
            joined = joined[:width] + joined[width:]
            totals[local] = jnp.concatenate(
                [joined[:, :width], joined[:, width:] + c["add"]], axis=1
            )
        query_here = query[rows, c["lanes"]]
        query_f = query_here.astype(f32)
        query_scale = lax.rsqrt(
            jnp.sum(query_f * query_f, axis=1, keepdims=True) + epsilon
        ) * (width ** (-0.5))
        gate = decay[pl.ds(c["head"], 1), :][:, rows]
        read_cum = jnp.sum(jnp.where(read_lane <= read_col, gate, 0.0), axis=1, keepdims=True)
        weights = jnp.exp(jnp.minimum(read_cum - c["cum_row"], read_mask[c["block"]]))
        weights = weights * dot_nt(query_here, c["key"]) * query_scale * c["scale_row"]
        writes_top = c["writes"].astype(bf16)
        seen = dot_nn(
            jnp.concatenate(halves(weights), axis=1),
            jnp.concatenate([writes_top, writes_top], axis=0),
        )
        read_carry = jnp.sum(
            jnp.where(read_step == read_col * refl, c["carry_row"], 0.0), axis=1, keepdims=True
        )
        offsets[local, rows, :] = seen[:, :width]
        reads[local, rows, :] = (
            (read_carry * query_scale) * query_f - seen[:, width:]
        ).astype(bf16)
    for local in range(heads_here):
        both = totals[local].astype(bf16)
        slot = (turn * heads_here + local) ^ place
        for other, send in enumerate(sends):

            @pl.when(slot == other)
            def _():
                send[...] = both

    @pl.when(turn == turns - 1)
    def _():
        for copy in passed:
            copy.wait()


def chosen(index, options):
    value = options[0]
    for other in range(1, len(options)):
        value = jnp.where(index == other, options[other], value)
    return value


def run_states(place, parts, state):
    states = []
    width = parts[0].shape[0]
    for member in range(len(parts)):
        states.append(state)
        both = chosen(place ^ member, [part[...] for part in parts])
        top = both[:, :width]
        added = both[:, width:].astype(f32)
        if state is None:
            state = added
        else:
            state = added + dot_nn(
                jnp.concatenate([top, top], axis=1), jnp.concatenate(halves(state), axis=0)
            )
    return states, state


def macro_kernel(*refs):
    count = len(refs) - 1
    place = lax.rem(lax.axis_index("seq"), count)
    states, state = run_states(place, refs[:count], None)
    refs[-1][...] = state.astype(bf16)


def settled(arrivals, count):
    macro = lax.axis_index("seq") // count
    last = jnp.clip(macro - 1, 0, len(arrivals) - 1)
    return chosen(last, [arrived[...] for arrived in arrivals]).astype(f32)


def hop_kernel(*refs, count):
    place = lax.rem(lax.axis_index("seq"), count)
    states, state = run_states(place, refs[-1 - count : -1], settled(refs[: -1 - count], count))
    refs[-1][...] = state.astype(bf16)


def spread_kernel(*refs, count):
    place = lax.rem(lax.axis_index("seq"), count)
    arrivals, parts, outs = refs[: -2 * count], refs[-2 * count : -count], refs[-count:]
    states, state = run_states(place, parts, settled(arrivals, count))
    states = [value.astype(bf16) for value in states]
    for turn in range(count):
        outs[turn][...] = chosen(place ^ turn, states)


def final_kernel(*refs):
    heads = refs[-1].shape[1] // refs[0].shape[1]
    first_states = refs[:heads]
    reads, offsets, maps, adds, gain, weight = refs[heads : heads + 6]
    outs, normed = refs[heads + 6 : -1], refs[-1]
    heads, tokens, width = reads.shape
    blocks = tokens // BLOCK
    place = lax.rem(lax.axis_index("seq"), heads)
    held = [ref[...] for ref in first_states]
    states = [chosen(place ^ head, held) for head in range(heads)]
    for block in range(blocks):
        at = block * BLOCK
        for head in range(heads):
            state = states[head]
            out = dot_nn(reads[head, at : at + BLOCK, :], state) + offsets[head, at : at + BLOCK, :]
            out = out * lax.rsqrt(jnp.mean(out * out, axis=1, keepdims=True) + epsilon)
            normed[at : at + BLOCK, head * width : (head + 1) * width] = (
                out * gain[...]
            ).astype(bf16)
            if block + 1 < blocks:
                states[head] = (dot_nn(maps[head, block], state) + adds[head, block]).astype(bf16)
    peers = len(outs)
    rows = tokens // peers
    me = lax.axis_index("head")
    for turn in range(peers):
        chunk = me ^ turn
        here = normed[pl.ds(pl.multiple_of(chunk * rows, rows), rows), :]
        outs[turn][...] = dot_nn(here, weight[...]).astype(bf16)


def exchanged(value, axis, mask):
    count = lax.axis_size(axis)
    return lax.ppermute(value, axis, [(source, source ^ mask) for source in range(count)])


def shifted(value, axis, steps, least=0):
    count = lax.axis_size(axis)
    pairs = [(source, source + steps) for source in range(least, count - steps)]
    return lax.ppermute(value, axis, pairs)


def grant(mebibytes):
    return pltpu.CompilerParams(vmem_limit_bytes=mebibytes << 20)


def body(
    queries,
    reflect_keys,
    reflect_values,
    reflect_beta,
    log_decay,
    prompt_lengths,
    norm_gain,
    out_weight,
):
    tokens = queries.shape[1]
    refl = reflect_keys.shape[2]
    heads = reflect_beta.shape[3]
    width = queries.shape[2] // heads
    blocks = tokens // BLOCK
    steps = refl * BLOCK
    beta = reflect_beta[0].transpose(1, 2, 0)
    decay = log_decay[0].transpose(1, 0)
    pair = HEADS_PER_STEP
    rows_spec = pl.BlockSpec((pair, tokens, width), lambda h: (h, 0, 0))
    square_spec = pl.BlockSpec((pair, blocks, width, width), lambda h: (h, 0, 0, 0))
    send_spec = pl.BlockSpec((width, 2 * width), lambda h: (0, 0))
    both_shape = jax.ShapeDtypeStruct((width, 2 * width), bf16)
    reads, offsets, maps, adds, weight, gain, *mine = pl.pallas_call(
        local_kernel,
        grid=(heads // pair,),
        in_specs=[pl.BlockSpec(memory_space=pltpu.HBM)] * 8,
        out_specs=[rows_spec, rows_spec, square_spec, square_spec]
        + [pl.BlockSpec(memory_space=pl.ANY)] * 2
        + [send_spec] * heads,
        out_shape=[
            jax.ShapeDtypeStruct((heads, tokens, width), bf16),
            jax.ShapeDtypeStruct((heads, tokens, width), f32),
            jax.ShapeDtypeStruct((heads, blocks, width, width), bf16),
            jax.ShapeDtypeStruct((heads, blocks, width, width), f32),
            jax.ShapeDtypeStruct(out_weight.shape, bf16),
            jax.ShapeDtypeStruct((1, width), f32),
        ]
        + [both_shape] * heads,
        scratch_shapes=[
            pltpu.VMEM((blocks, steps, steps), f32),
            pltpu.VMEM((blocks, BLOCK, steps), f32),
            pltpu.VMEM((blocks, 8, steps), f32),
            pltpu.SMEM(prompt_lengths.shape, jnp.int32),
            pltpu.VMEM((heads // pair, tokens, pair * width), bf16),
            pltpu.VMEM((heads // pair, tokens, refl, pair * width), bf16),
            pltpu.VMEM((heads // pair, tokens, refl, pair * width), bf16),
            pltpu.VMEM(beta.shape, f32),
            pltpu.VMEM(decay.shape, f32),
            pltpu.SemaphoreType.DMA((5 + 3 * (heads // pair),)),
        ],
        compiler_params=grant(20),
        name="local_blocks",
    )(
        *[
            pltpu.with_memory_space_constraint(array, pltpu.HBM)
            for array in (prompt_lengths, queries, reflect_keys, reflect_values, beta, decay)
            + (out_weight, norm_gain[None])
        ]
    )

    state_shape = jax.ShapeDtypeStruct((width, width), bf16)
    parts = [mine[0]] + [exchanged(mine[r], "seq", r) for r in range(1, heads)]
    sent = pl.pallas_call(
        macro_kernel, out_shape=state_shape, compiler_params=grant(4), name="macro"
    )(*parts)
    macro_hops = -(-(MOST_LEN - 1) // (tokens * heads))
    arrivals = [shifted(sent, "seq", heads)]
    for hop in range(1, macro_hops):
        sent = pl.pallas_call(
            functools.partial(hop_kernel, count=heads),
            out_shape=state_shape,
            compiler_params=grant(4),
            name="hop",
        )(*arrivals, *parts)
        arrivals.append(shifted(sent, "seq", heads, hop * heads))
    given = pl.pallas_call(
        functools.partial(spread_kernel, count=heads),
        out_shape=[state_shape] * heads,
        compiler_params=grant(4),
        name="spread",
    )(*arrivals, *parts)
    states = [given[0]] + [exchanged(given[r], "seq", r) for r in range(1, heads)]

    peers = lax.axis_size("head")
    rows = tokens // peers
    pieces = pl.pallas_call(
        final_kernel,
        out_shape=[jax.ShapeDtypeStruct((rows, out_weight.shape[1]), bf16)] * peers,
        scratch_shapes=[pltpu.VMEM((tokens, heads * width), bf16)],
        compiler_params=grant(16),
        name="read_and_project",
    )(*states, reads, offsets, maps, adds, gain, weight)
    total = pieces[0].astype(f32)
    for turn in (2, 1, 3):
        total = total + exchanged(pieces[turn], "head", turn).astype(f32)
    return total.astype(bf16)[None]


def solution(mesh):
    in_specs = (
        P(("parts", "rep"), "seq", "head"),
        P(("parts", "rep"), "seq", None, "head"),
        P(("parts", "rep"), "seq", None, "head"),
        P(("parts", "rep"), "seq", None, "head"),
        P(("parts", "rep"), "seq", "head"),
        P(("parts", "rep"), None),
        P(),
        P("head", None),
    )
    out_specs = P(("parts", "rep"), ("seq", "head"), None)
    return jax.shard_map(body, mesh=mesh, in_specs=in_specs, out_specs=out_specs, check_vma=False)
```

```python
import functools

import jax
import jax.numpy as jnp
from jax import lax
from jax.experimental import pallas as pl
from jax.experimental.pallas import tpu as pltpu
from jax.sharding import PartitionSpec as P

BLOCK = 64
HEADS_PER_STEP = 4
epsilon = 1e-06
f32 = jnp.float32
bf16 = jnp.bfloat16


def dot_nn(left, right):
    return lax.dot_general(left, right, (((1,), (0,)), ((), ())), preferred_element_type=f32)


def dot_nt(left, right):
    return lax.dot_general(left, right, (((1,), (1,)), ((), ())), preferred_element_type=f32)


def dot_tn(left, right):
    return lax.dot_general(left, right, (((0,), (0,)), ((), ())), preferred_element_type=f32)


def halves(value):
    top = value.astype(bf16)
    return top, (value - top.astype(f32)).astype(bf16)


def square_product(left, right):
    width = right[0].shape[1]
    side = jnp.concatenate([right[0], right[1]], axis=1)
    both = dot_nn(
        jnp.concatenate([left[0], left[1]], axis=1), jnp.concatenate([side, side], axis=0)
    )
    return both[:, :width] + both[:, width:]


def iota(shape, dim):
    return lax.broadcasted_iota(jnp.int32, shape, dim)


def local_kernel(
    far_lengths, far_query, far_keys, far_values, far_beta, far_decay, far_weight, far_gain, reads, offsets, maps, adds, *rest
):
    weight, gain = rest[:2]
    sends = rest[2:-10]
    inner_mask, read_mask, edge_mask = rest[-10:-7]
    lengths, query_all, keys_all, values_all, beta, decay, done = rest[-7:]
    turns = query_all.shape[0]
    tokens = query_all.shape[1]
    heads_here = reads.shape[0] // turns
    width = reads.shape[2]
    refl = keys_all.shape[2]
    steps = BLOCK * refl
    blocks = tokens // BLOCK
    first = lax.axis_index("seq") * tokens
    place = lax.rem(lax.axis_index("seq"), len(sends))
    row = iota((steps, steps), 0)
    col = iota((steps, steps), 1)
    eye = row == col
    unit = jnp.where(eye, 1.0, 0.0).astype(f32)
    step_col = iota((steps, 1), 0)
    token_col = step_col // refl
    refl_col = step_col % refl
    token_lane = iota((steps, BLOCK), 1)
    token_row = iota((1, steps), 1) // refl
    read_col = iota((BLOCK, 1), 0)
    read_lane = iota((BLOCK, BLOCK), 1)
    read_step = iota((BLOCK, steps), 1)
    read_token = read_step // refl
    hidden = -1e30

    span = heads_here * width
    copies = [
        pltpu.make_async_copy(source, target, done.at[index])
        for index, (source, target) in enumerate(
            [(far_lengths, lengths), (far_decay, decay), (far_beta, beta)]
        )
    ]

    passed = [
        pltpu.make_async_copy(source, target, done.at[3 + 3 * turns + index])
        for index, (source, target) in enumerate([(far_weight, weight), (far_gain, gain)])
    ]

    def fetch(kind, part):
        lanes = pl.ds(part * span, span)
        source, target = [
            (far_keys.at[0, :, :, lanes], keys_all.at[part]),
            (far_values.at[0, :, :, lanes], values_all.at[part]),
            (far_query.at[0, :, lanes], query_all.at[part]),
        ][kind]
        return pltpu.make_async_copy(source, target, done.at[3 + kind * turns + part])

    for copy in copies:
        copy.start()
    for part in range(turns):
        for kind in range(3):
            fetch(kind, part).start()
    for copy in passed:
        copy.start()
    for copy in copies:
        copy.wait()
    ends, end = [], jnp.int32(0)
    for doc in range(lengths.shape[1]):
        end = end + lengths[0, doc]
        ends.append(end)

    def start_of(position):
        start = jnp.zeros_like(position)
        for end in ends:
            start = jnp.where(end <= position, end, start)
        return start

    for block in range(blocks):
        begin = first + block * BLOCK
        start = start_of(begin + token_col)
        inner_mask[block] = jnp.where(
            (col < row) & (begin + col // refl >= start), 0.0, hidden
        )
        read_start = start_of(begin + read_col)
        read_mask[block] = jnp.where(
            (read_token <= read_col) & (begin + read_token >= read_start), 0.0, hidden
        )
        start_row = start_of(begin + token_row)
        last_start = start_of(begin + token_row * 0 + (BLOCK - 1))
        edge_mask[block, 0:1, :] = jnp.where(start_row < begin, 0.0, hidden)
        edge_mask[block, 1:2, :] = jnp.where(begin + token_row >= last_start, 0.0, hidden)

    def to_row(column):
        return jnp.sum(jnp.where(eye, column, 0.0), axis=0, keepdims=True)

    def to_col(line):
        return jnp.sum(jnp.where(eye, line, 0.0), axis=1, keepdims=True)

    def run(turn, unused):
        keys, values, query = keys_all.at[turn], values_all.at[turn], query_all.at[turn]
        for kind in range(3):
            fetch(kind, turn).wait()
        chains = []
        for block in range(blocks):
            for local in range(heads_here):
                lanes = slice(local * width, (local + 1) * width)
                at = block * BLOCK
                rows = slice(at, at + BLOCK)
                chains.append(
                    dict(
                        local=local,
                        block=block,
                        rows=rows,
                        lanes=lanes,
                        head=turn * heads_here + local,
                        key=keys[rows, :, lanes].reshape(steps, width),
                    )
                )
        for c in chains:
            c["gram"] = dot_nt(c["key"], c["key"])
        for c in chains:
            gate = decay[pl.ds(c["head"], 1), :][:, c["rows"]]
            cum = jnp.sum(jnp.where(token_lane <= token_col, gate, 0.0), axis=1, keepdims=True)
            beta_here = beta[refl - 1, pl.ds(c["head"], 1), :][:, c["rows"]]
            for j in range(refl - 1):
                beta_here = jnp.where(
                    refl_col == j, beta[j, pl.ds(c["head"], 1), :][:, c["rows"]], beta_here
                )
            c["cum"] = cum
            c["strength"] = jnp.sum(
                jnp.where(token_lane == token_col, beta_here, 0.0), axis=1, keepdims=True
            )
        for c in chains:
            diagonal = jnp.where(eye, c["gram"], 0.0)
            c["scale"] = lax.rsqrt(jnp.sum(diagonal, axis=1, keepdims=True) + epsilon)
            c["scale_row"] = lax.rsqrt(jnp.sum(diagonal, axis=0, keepdims=True) + epsilon)
            c["cum_row"] = to_row(c["cum"])
            c["strength_row"] = to_row(c["strength"])
        for c in chains:
            ratio = jnp.exp(jnp.minimum(c["cum"] - c["cum_row"], inner_mask[c["block"]]))
            system = (c["strength"] * c["scale"]) * ratio * c["gram"] * c["scale_row"]
            c["system"] = halves(system)
            c["inverse"] = unit - jnp.where((row ^ col) == 1, system, 0.0)
        size = 2
        while size < steps:
            mask = ((row // size) ^ (col // size)) == 1
            for c in chains:
                c["halves"] = halves(c["inverse"])
                corner = tuple(jnp.where(mask, part, jnp.zeros_like(part)) for part in c["system"])
                c["moved"] = square_product(corner, c["halves"])
            for c in chains:
                c["inverse"] = c["inverse"] - square_product(c["halves"], halves(c["moved"]))
            size *= 2
        for c in chains:
            value = values[c["rows"], :, c["lanes"]].reshape(steps, width)
            carry_row = jnp.exp(jnp.minimum(c["cum_row"], edge_mask[c["block"], 0:1, :]))
            c["carry_row"] = carry_row
            value_side = jnp.concatenate(halves(c["inverse"] * c["strength_row"]), axis=1)
            key_side = jnp.concatenate(
                halves(c["inverse"] * (c["strength_row"] * carry_row * c["scale_row"])), axis=1
            )
            c["twice"] = jnp.concatenate([c["key"], c["key"]], axis=0)
            c["writes"] = jnp.concatenate(
                [
                    dot_nn(value_side, jnp.concatenate([value, value], axis=0)),
                    dot_nn(key_side, c["twice"]),
                ],
                axis=1,
            )
        for c in chains:
            cum_row = c["cum_row"]
            fade_row = c["scale_row"] * jnp.exp(
                jnp.minimum(cum_row[:, steps - 1 :] - cum_row, edge_mask[c["block"], 1:2, :])
            )
            faded = jnp.concatenate(halves(to_col(fade_row) * c["writes"]), axis=0)
            summed = dot_tn(c["twice"], faded)
            c["add"] = summed[:, :width]
            c["map"] = c["carry_row"][:, steps - 1 :] * unit - summed[:, width:]
        for c in chains:
            maps[c["head"], c["block"]] = c["map"].astype(bf16)
            adds[c["head"], c["block"]] = c["add"]
        totals = [None] * heads_here
        for c in chains:
            local, rows = c["local"], c["rows"]
            if totals[local] is None:
                totals[local] = jnp.concatenate([c["map"], c["add"]], axis=1)
            else:
                top, low = halves(c["map"])
                tall = jnp.concatenate(
                    [
                        jnp.concatenate([top, top], axis=1),
                        jnp.concatenate([low, jnp.zeros_like(low)], axis=1),
                    ],
                    axis=0,
                )
                joined = dot_nn(tall, jnp.concatenate(halves(totals[local]), axis=0))
                joined = joined[:width] + joined[width:]
                totals[local] = jnp.concatenate(
                    [joined[:, :width], joined[:, width:] + c["add"]], axis=1
                )
        for c in chains:
            local, rows = c["local"], c["rows"]
            query_here = query[rows, c["lanes"]]
            query_f = query_here.astype(f32)
            query_scale = lax.rsqrt(
                jnp.sum(query_f * query_f, axis=1, keepdims=True) + epsilon
            ) * (width ** (-0.5))
            gate = decay[pl.ds(c["head"], 1), :][:, rows]
            read_cum = jnp.sum(jnp.where(read_lane <= read_col, gate, 0.0), axis=1, keepdims=True)
            weights = jnp.exp(jnp.minimum(read_cum - c["cum_row"], read_mask[c["block"]]))
            weights = weights * dot_nt(query_here, c["key"]) * query_scale * c["scale_row"]
            writes_top = c["writes"].astype(bf16)
            seen = dot_nn(
                jnp.concatenate(halves(weights), axis=1),
                jnp.concatenate([writes_top, writes_top], axis=0),
            )
            read_carry = jnp.sum(
                jnp.where(read_step == read_col * refl, c["carry_row"], 0.0), axis=1, keepdims=True
            )
            offsets[c["head"], rows, :] = seen[:, :width]
            reads[c["head"], rows, :] = (
                (read_carry * query_scale) * query_f - seen[:, width:]
            ).astype(bf16)
        for local in range(heads_here):
            both = totals[local].astype(bf16)
            slot = (turn * heads_here + local) ^ place
            for other, send in enumerate(sends):

                @pl.when(slot == other)
                def _():
                    send[...] = both
        return unused

    lax.fori_loop(0, turns, run, 0)
    for copy in passed:
        copy.wait()


def chosen(index, options):
    value = options[0]
    for other in range(1, len(options)):
        value = jnp.where(index == other, options[other], value)
    return value


def run_states(place, parts, state):
    states = []
    width = parts[0].shape[0]
    for member in range(len(parts)):
        states.append(state)
        both = chosen(place ^ member, [part[...] for part in parts])
        top = both[:, :width]
        added = both[:, width:].astype(f32)
        if state is None:
            state = added
        else:
            state = added + dot_nn(
                jnp.concatenate([top, top], axis=1), jnp.concatenate(halves(state), axis=0)
            )
    return states, state


def macro_kernel(*refs):
    count = len(refs) - 1
    place = lax.rem(lax.axis_index("seq"), count)
    states, state = run_states(place, refs[:count], None)
    refs[-1][...] = state.astype(bf16)


def settled(arrivals, count):
    macro = lax.axis_index("seq") // count
    last = jnp.clip(macro - 1, 0, len(arrivals) - 1)
    return chosen(last, [arrived[...] for arrived in arrivals]).astype(f32)


def hop_kernel(*refs, count):
    place = lax.rem(lax.axis_index("seq"), count)
    states, state = run_states(place, refs[-1 - count : -1], settled(refs[: -1 - count], count))
    refs[-1][...] = state.astype(bf16)


def spread_kernel(*refs, count):
    place = lax.rem(lax.axis_index("seq"), count)
    arrivals, parts, outs = refs[: -2 * count], refs[-2 * count : -count], refs[-count:]
    states, state = run_states(place, parts, settled(arrivals, count))
    states = [value.astype(bf16) for value in states]
    for turn in range(count):
        outs[turn][...] = chosen(place ^ turn, states)


def final_kernel(*refs):
    heads = refs[-1].shape[1] // refs[0].shape[1]
    first_states = refs[:heads]
    reads, offsets, maps, adds, gain, weight = refs[heads : heads + 6]
    outs, normed = refs[heads + 6 : -1], refs[-1]
    heads, tokens, width = reads.shape
    blocks = tokens // BLOCK
    place = lax.rem(lax.axis_index("seq"), heads)
    held = [ref[...] for ref in first_states]
    states = [chosen(place ^ head, held) for head in range(heads)]
    for block in range(blocks):
        at = block * BLOCK
        for head in range(heads):
            state = states[head]
            out = dot_nn(reads[head, at : at + BLOCK, :], state) + offsets[head, at : at + BLOCK, :]
            out = out * lax.rsqrt(jnp.mean(out * out, axis=1, keepdims=True) + epsilon)
            normed[at : at + BLOCK, head * width : (head + 1) * width] = (
                out * gain[...]
            ).astype(bf16)
            if block + 1 < blocks:
                states[head] = (dot_nn(maps[head, block], state) + adds[head, block]).astype(bf16)
    peers = len(outs)
    rows = tokens // peers
    me = lax.axis_index("head")
    for turn in range(peers):
        chunk = me ^ turn
        here = normed[pl.ds(pl.multiple_of(chunk * rows, rows), rows), :]
        outs[turn][...] = dot_nn(here, weight[...]).astype(bf16)


def exchanged(value, axis, mask):
    count = lax.axis_size(axis)
    return lax.ppermute(value, axis, [(source, source ^ mask) for source in range(count)])


def passed_on(value, axis, size, row):
    pairs = [(row * size + member, (row + 1) * size + member) for member in range(size)]
    return lax.ppermute(value, axis, pairs)


def grant(mebibytes):
    return pltpu.CompilerParams(vmem_limit_bytes=mebibytes << 20)


def body(
    queries,
    reflect_keys,
    reflect_values,
    reflect_beta,
    log_decay,
    prompt_lengths,
    norm_gain,
    out_weight,
):
    tokens = queries.shape[1]
    refl = reflect_keys.shape[2]
    heads = reflect_beta.shape[3]
    width = queries.shape[2] // heads
    blocks = tokens // BLOCK
    steps = refl * BLOCK
    beta = reflect_beta[0].transpose(1, 2, 0)
    decay = log_decay[0].transpose(1, 0)
    pair = HEADS_PER_STEP
    both_shape = jax.ShapeDtypeStruct((width, 2 * width), bf16)
    reads, offsets, maps, adds, weight, gain, *mine = pl.pallas_call(
        local_kernel,
        in_specs=[pl.BlockSpec(memory_space=pltpu.HBM)] * 8,
        out_specs=[pl.BlockSpec(memory_space=pltpu.VMEM)] * 4
        + [pl.BlockSpec(memory_space=pl.ANY)] * 2
        + [pl.BlockSpec(memory_space=pltpu.VMEM)] * heads,
        out_shape=[
            jax.ShapeDtypeStruct((heads, tokens, width), bf16),
            jax.ShapeDtypeStruct((heads, tokens, width), f32),
            jax.ShapeDtypeStruct((heads, blocks, width, width), bf16),
            jax.ShapeDtypeStruct((heads, blocks, width, width), f32),
            jax.ShapeDtypeStruct(out_weight.shape, bf16),
            jax.ShapeDtypeStruct((1, width), f32),
        ]
        + [both_shape] * heads,
        scratch_shapes=[
            pltpu.VMEM((blocks, steps, steps), f32),
            pltpu.VMEM((blocks, BLOCK, steps), f32),
            pltpu.VMEM((blocks, 8, steps), f32),
            pltpu.SMEM(prompt_lengths.shape, jnp.int32),
            pltpu.VMEM((heads // pair, tokens, pair * width), bf16),
            pltpu.VMEM((heads // pair, tokens, refl, pair * width), bf16),
            pltpu.VMEM((heads // pair, tokens, refl, pair * width), bf16),
            pltpu.VMEM(beta.shape, f32),
            pltpu.VMEM(decay.shape, f32),
            pltpu.SemaphoreType.DMA((5 + 3 * (heads // pair),)),
        ],
        compiler_params=grant(20),
        name="local_blocks",
    )(
        *[
            pltpu.with_memory_space_constraint(array, pltpu.HBM)
            for array in (prompt_lengths, queries, reflect_keys, reflect_values, beta, decay)
            + (out_weight, norm_gain[None])
        ]
    )

    state_shape = jax.ShapeDtypeStruct((width, width), bf16)
    parts = [mine[0]] + [exchanged(mine[r], "seq", r) for r in range(1, heads)]
    sent = pl.pallas_call(
        macro_kernel, out_shape=state_shape, compiler_params=grant(4), name="macro"
    )(*parts)
    arrivals = [passed_on(sent, "seq", heads, 0)]
    for hop in range(1, lax.axis_size("seq") // heads - 1):
        sent = pl.pallas_call(
            functools.partial(hop_kernel, count=heads),
            out_shape=state_shape,
            compiler_params=grant(4),
            name="hop",
        )(*arrivals, *parts)
        arrivals.append(passed_on(sent, "seq", heads, hop))
    given = pl.pallas_call(
        functools.partial(spread_kernel, count=heads),
        out_shape=[state_shape] * heads,
        compiler_params=grant(4),
        name="spread",
    )(*arrivals, *parts)
    states = [given[0]] + [exchanged(given[r], "seq", r) for r in range(1, heads)]

    peers = lax.axis_size("head")
    rows = tokens // peers
    pieces = pl.pallas_call(
        final_kernel,
        out_shape=[jax.ShapeDtypeStruct((rows, out_weight.shape[1]), bf16)] * peers,
        scratch_shapes=[pltpu.VMEM((tokens, heads * width), bf16)],
        compiler_params=grant(16),
        name="read_and_project",
    )(*states, reads, offsets, maps, adds, gain, weight)
    total = pieces[0].astype(f32)
    for turn in (2, 1, 3):
        total = total + exchanged(pieces[turn], "head", turn).astype(f32)
    return total.astype(bf16)[None]


def solution(mesh):
    in_specs = (
        P(("parts", "rep"), "seq", "head"),
        P(("parts", "rep"), "seq", None, "head"),
        P(("parts", "rep"), "seq", None, "head"),
        P(("parts", "rep"), "seq", None, "head"),
        P(("parts", "rep"), "seq", "head"),
        P(("parts", "rep"), None),
        P(),
        P("head", None),
    )
    out_specs = P(("parts", "rep"), ("seq", "head"), None)
    return jax.shard_map(body, mesh=mesh, in_specs=in_specs, out_specs=out_specs, check_vma=False)
```
